128 devices in a mesh: ctx: 16 (over z, x_lo, core), tp: 8 (over x_hi, y).
Axes of the slice: x: 4 (x_hi: 2, x_lo: 2; x = x_hi * 2 + x_lo), y: 4, z: 4, core: 2. Of those that a mesh axis runs over, the one named last changes fastest.
Arguments:
- tokens: bfloat16 [2, 4096, 8192], P(None, 'ctx', 'tp'), may hold values from -14 to 14
- norm_gain: float32 [8192], replicated, may hold values from 0.5 to 1.5
- span_order: int32 [2, 32], replicated, may hold values from 0 to 31, each once within a row
- w_query: bfloat16 [8192, 4096], P('ctx', 'tp'), may hold values from -0.10122281 to 0.10122281
- w_key: bfloat16 [8192, 1024], P('ctx', 'tp'), may hold values from -0.10122281 to 0.10122281
- value_weight: bfloat16 [8192, 1024], P('ctx', 'tp'), may hold values from -0.0625 to 0.0625
- w_out: bfloat16 [4096, 8192], P('tp', 'ctx'), may hold values from -0.75 to 0.75
Outputs:
- mixed: bfloat16 [2, 4096, 8192], P(None, 'ctx', 'tp')
The draws below stay inside these ranges and needn't reach their ends.
Inputs may be any that keep to these rules, and one draw needn't show every extreme that they name: Each row of span_order names every one of the 2 * 16 blocks of positions once; stored block b of a sequence holds positions span_order[b] * 128 onwards, in order.
All inputs are finite; a program needn't handle non-finite values.
Results may differ from the reference program's by a relative error of at most 0.014.
Values may be sent and summed in bfloat16 or wider, within the bound.
A program may use at most 128 MiB of HBM per device.

```python
import math
import jax
import jax.numpy as jnp
from jax import lax

MODEL_WIDTH = 8192
QUERY_HEAD_COUNT = 32
KEY_VALUE_HEADS = 8
HEAD_DIM = 128
SEQUENCE_LENGTH = 4096
SEQS = 2
N_CTX = 16
N_TP = 8


def unscaled_weight(key, salt, columns):
    spread = (2.0 / MODEL_WIDTH) ** 0.5
    normal_part = jax.random.normal(jax.random.fold_in(key, salt), (MODEL_WIDTH, columns), jnp.float32)
    return jnp.clip(normal_part, -6.0, 6.0) * spread


def draw_w_query(key, part):
    weight_portion = unscaled_weight(key, 11, QUERY_HEAD_COUNT * HEAD_DIM)
    return weight_portion.astype(jnp.bfloat16)


def draw_w_key(key, part):
    weight_portion = unscaled_weight(key, 12, KEY_VALUE_HEADS * HEAD_DIM)
    return weight_portion.astype(jnp.bfloat16)


def draw_tokens(key, part):
    noise_part = jnp.clip(jax.random.normal(jax.random.fold_in(key, 13), (SEQS, SEQUENCE_LENGTH, MODEL_WIDTH), jnp.float32), -6.0, 6.0)
    return noise_part.astype(jnp.bfloat16)


def level_of(key, extent, cuts, smallest, high):
    loudness = 1.0
    for axis_at, parts in cuts:
        draws = jax.random.uniform(jax.random.fold_in(jax.random.fold_in(key, 6), axis_at), (parts,), jnp.float32, smallest / len(cuts), high / len(cuts))
        loudness = loudness * jnp.repeat(jnp.exp(draws), extent[axis_at] // parts).reshape((-1,) + (1,) * (len(extent) - 1 - axis_at))
    return loudness


def noise(rng, shape, deviation, reach, cuts=(), kind=jnp.bfloat16):
    array = deviation * jax.random.normal(rng, shape, jnp.float32)
    if cuts:
        array = array * level_of(rng, shape, cuts, -0.22, 0.18)
    return jnp.clip(array, -reach, reach).astype(kind)


def setup_inputs(seed: int = 0) -> dict:
    splits = jax.random.split(jax.random.key(seed), 8)
    return {
        "tokens": draw_tokens(jax.random.fold_in(splits[7], 71), 0),
        "norm_gain": jnp.clip(1.0 + 0.1 * jax.random.normal(splits[1], (MODEL_WIDTH,), jnp.float32), 0.5, 1.5),
        "span_order": jax.vmap(lambda own: jax.random.permutation(own, 2 * N_CTX))(jax.random.split(splits[2], SEQS)).reshape((SEQS, 2 * N_CTX)).astype(jnp.int32),
        "w_query": draw_w_query(jax.random.fold_in(splits[7], 71), 0),
        "w_key": draw_w_key(jax.random.fold_in(splits[7], 71), 0),
        "value_weight": noise(splits[5], (MODEL_WIDTH, KEY_VALUE_HEADS * HEAD_DIM), MODEL_WIDTH ** -0.5, 0.0625, ((0, 16), (1, 8))),
        "w_out": noise(splits[6], (QUERY_HEAD_COUNT * HEAD_DIM, MODEL_WIDTH), (QUERY_HEAD_COUNT * HEAD_DIM // 64) ** -0.5, 0.75, ((0, 8), (1, 16))),
    }


theta_base = 500000.0
norm_eps = 1e-05
masked_score = -1e+30

def normalize(flat_rows, norm_gain):
    wide = flat_rows.astype(jnp.float32)
    factor = lax.rsqrt(lax.optimization_barrier(jnp.mean(wide * wide, axis=-1, keepdims=True)) + norm_eps)
    return (wide * factor * norm_gain).astype(jnp.bfloat16)

def positions_of(span_order, first, count, block_rows):
    stored = first + jnp.arange(count, dtype=jnp.int32)
    which = stored // block_rows
    slots = jnp.arange(span_order.shape[1], dtype=jnp.int32)
    picked = lax.optimization_barrier(jnp.sum(jnp.where(slots[None, None, :] == which[None, :, None], span_order[:, None, :], 0), axis=2))
    return (picked * block_rows + stored % block_rows).astype(jnp.int32)

def apply_rotation(value_rows, token_position, head_size):
    half = head_size // 2
    freqs = jnp.exp(-(2.0 * jnp.arange(half, dtype=jnp.float32) / head_size) * math.log(theta_base))
    angle = token_position.astype(jnp.float32)[..., None] * freqs
    cosine = jnp.cos(angle)[:, :, None, :]
    sine = jnp.sin(angle)[:, :, None, :]
    front = value_rows[..., :half]
    back = value_rows[..., half:]
    return jnp.concatenate([front * cosine - back * sine, back * cosine + front * sine], axis=-1)

def reference(tokens, norm_gain, span_order, w_query, w_key, value_weight, w_out):
    sequence_batch = tokens.shape[0]
    token_length = tokens.shape[1]
    block_rows = token_length // (2 * N_CTX)
    normed = normalize(tokens.reshape(sequence_batch * token_length, MODEL_WIDTH), norm_gain)
    token_position = positions_of(span_order, 0, token_length, block_rows)
    query_flat = jnp.dot(normed, w_query, preferred_element_type=jnp.float32)
    flattened_key = jnp.dot(normed, w_key, preferred_element_type=jnp.float32)
    flattened_value = jnp.dot(normed, value_weight, preferred_element_type=jnp.float32)
    query = apply_rotation(query_flat.reshape(sequence_batch, token_length, QUERY_HEAD_COUNT, HEAD_DIM), token_position, HEAD_DIM).astype(jnp.bfloat16)
    key_rows = apply_rotation(flattened_key.reshape(sequence_batch, token_length, KEY_VALUE_HEADS, HEAD_DIM), token_position, HEAD_DIM).astype(jnp.bfloat16)
    value_rows = flattened_value.reshape(sequence_batch, token_length, KEY_VALUE_HEADS, HEAD_DIM).astype(jnp.bfloat16)
    group_width = QUERY_HEAD_COUNT // KEY_VALUE_HEADS
    factor = 1.0 / math.sqrt(HEAD_DIM)
    allowed = token_position[:, None, :] <= token_position[:, :, None]

    def single_head(head):
        query_block = lax.dynamic_slice_in_dim(query, (head * group_width).astype(jnp.int32), group_width, 2).astype(jnp.float32)
        key_block = lax.dynamic_slice_in_dim(key_rows, head.astype(jnp.int32), 1, 2)[:, :, 0, :].astype(jnp.float32)
        value_block = lax.dynamic_slice_in_dim(value_rows, head.astype(jnp.int32), 1, 2)[:, :, 0, :].astype(jnp.float32)
        scores = jnp.einsum('sqgd,skd->sgqk', query_block, key_block) * factor
        scores = jnp.where(allowed[:, None], scores, masked_score)
        peak = lax.optimization_barrier(jnp.max(scores, axis=-1, keepdims=True))
        weights = jnp.where(allowed[:, None], jnp.exp(scores - peak), 0.0)
        total = lax.optimization_barrier(jnp.sum(weights, axis=-1))
        rounded = lax.optimization_barrier(weights.astype(jnp.bfloat16)).astype(jnp.float32)
        summed = jnp.einsum('sgqk,skd->sqgd', rounded, value_block)
        return (summed / jnp.transpose(total, (0, 2, 1))[..., None]).astype(jnp.bfloat16)
    head_outputs = lax.map(single_head, jnp.arange(KEY_VALUE_HEADS, dtype=jnp.int32))
    attended = jnp.transpose(head_outputs, (1, 2, 0, 3, 4)).reshape(sequence_batch * token_length, QUERY_HEAD_COUNT * HEAD_DIM)
    columns = QUERY_HEAD_COUNT * HEAD_DIM // N_TP
    summed = jnp.zeros((sequence_batch * token_length, MODEL_WIDTH), jnp.float32)
    for group in range(N_TP):
        partial_value = jnp.dot(attended[:, group * columns:(group + 1) * columns], w_out[group * columns:(group + 1) * columns], preferred_element_type=jnp.float32)
        summed = summed + lax.optimization_barrier(partial_value.astype(jnp.bfloat16)).astype(jnp.float32)
    return summed.astype(jnp.bfloat16).reshape(sequence_batch, token_length, MODEL_WIDTH)
```

```python
import math

import jax
import jax.numpy as jnp
from jax import lax
from jax.experimental import pallas as pl
from jax.experimental.pallas import tpu as pltpu
from jax.sharding import PartitionSpec as P

HEAD_DIM = 128


theta_base = 500000.0
norm_eps = 1e-05
masked_score = -1e30


def in_one_piece(arrays, axis, dim, along):
    ends, at = ([], 0)
    for a in arrays[:-1]:
        at += a.shape[along]
        ends.append(at)
    both = jnp.concatenate(arrays, axis=along)
    return tuple(jnp.split(lax.all_gather(both, axis, axis=dim, tiled=True), ends, axis=along))


def positions_of(span_order, first, count, block_rows):
    stored = first + jnp.arange(count, dtype=jnp.int32)
    which = stored // block_rows
    slots = jnp.arange(span_order.shape[1], dtype=jnp.int32)
    picked = jnp.sum(
        jnp.where(slots[None, None, :] == which[None, :, None], span_order[:, None, :], 0), axis=2
    )
    return picked * block_rows + stored % block_rows


def angles(token_position):
    half = HEAD_DIM // 2
    freqs = jnp.exp(-(2.0 * jnp.arange(half, dtype=jnp.float32) / HEAD_DIM) * math.log(theta_base))
    angle = token_position.astype(jnp.float32)[..., None] * freqs
    cosine, sine = jnp.cos(angle), jnp.sin(angle)
    return jnp.concatenate([cosine, cosine], axis=-1), jnp.concatenate([-sine, sine], axis=-1)


MESH = pl.DeviceIdType.MESH


def neighbours():
    ctx, tp = lax.axis_index("ctx"), lax.axis_index("tp")
    z, xl, core = ctx // 4, (ctx // 2) % 2, ctx % 2
    xh, y = tp // 4, tp % 4

    def at(z_, xl_, core_, xh_, y_):
        return {"ctx": z_ * 4 + xl_ * 2 + core_, "tp": xh_ * 4 + y_}

    return {
        "yp": at(z, xl, core, xh, (y + 1) % 4),
        "ym": at(z, xl, core, xh, (y + 3) % 4),
        "xh": at(z, xl, core, 1 - xh, y),
        "zp": at((z + 1) % 4, xl, core, xh, y),
        "zm": at((z + 3) % 4, xl, core, xh, y),
        "xl": at(z, 1 - xl, core, xh, y),
        "co": at(z, xl, 1 - core, xh, y),
    }


class Links:
    def __init__(self, send, recv):
        self.send, self.recv, self.count = send, recv, 0
        self.where = neighbours()
        self.sent = []

    def greet(self, names):
        barrier = pltpu.get_barrier_semaphore()
        for name in names:
            pl.semaphore_signal(barrier, 1, device_id=self.where[name], device_id_type=MESH)
        pl.semaphore_wait(barrier, len(names))

    def ticket(self):
        self.count += 1
        return self.count - 1

    def copy(self, ticket, src, dst, name):
        return pltpu.make_async_remote_copy(
            src, dst, self.send.at[ticket], self.recv.at[ticket],
            device_id=self.where[name], device_id_type=MESH,
        )

    def start(self, ticket, src, dst, name):
        c = self.copy(ticket, src, dst, name)
        c.start()
        self.sent.append(c)

    def arrive(self, ticket, here, name="co"):
        self.copy(ticket, here, here, name).wait_recv()

    def finish(self):
        for c in self.sent:
            c.wait_send()
        self.sent = []


def token_flow(links, tokens_buf, source):
    tp = lax.axis_index("tp")
    xh, y = tp // 4, tp % 4

    def shard(dx, dy):
        return (xh if dx == 0 else 1 - xh) * 4 + (y + dy) % 4

    def slot(dx, dy, s, rows=None):
        ref = tokens_buf.at[shard(dx, dy) * 2 + s]
        return ref if rows is None else ref.at[pl.ds(rows[0], rows[1])]

    events = []
    rows = tokens_buf.shape[1]
    low, high = (0, rows // 2), (rows // 2, rows // 2)
    T = {}
    for s in range(2):
        for k in ("yp", "ym", "xh", "fa", "fb", "pyp", "pym", "x2"):
            T[k, s] = links.ticket()

    def own(s):
        links.start(T["xh", s], source.at[s], slot(0, 0, s), "xh")
        links.start(T["yp", s], source.at[s], slot(0, 0, s), "yp")
        links.start(T["ym", s], source.at[s], slot(0, 0, s), "ym")

    def forward(s):
        links.arrive(T["yp", s], slot(0, 3, s), "ym")
        links.start(T["fa", s], slot(0, 3, s, low), slot(0, 3, s, low), "yp")
        links.arrive(T["ym", s], slot(0, 1, s), "yp")
        links.start(T["fb", s], slot(0, 1, s, high), slot(0, 1, s, high), "ym")

    def partner(s):
        links.arrive(T["xh", s], slot(1, 0, s), "xh")
        links.start(T["pyp", s], slot(1, 0, s), slot(1, 0, s), "yp")
        links.start(T["pym", s], slot(1, 0, s), slot(1, 0, s), "ym")

    def across(s):
        links.arrive(T["fa", s], slot(0, 2, s, low), "ym")
        links.arrive(T["fb", s], slot(0, 2, s, high), "yp")
        links.start(T["x2", s], slot(0, 2, s), slot(0, 2, s), "xh")

    def sides(s):
        links.arrive(T["pyp", s], slot(1, 3, s), "ym")
        links.arrive(T["pym", s], slot(1, 1, s), "yp")

    def last(s):
        links.arrive(T["x2", s], slot(1, 2, s), "xh")

    return dict(own=own, forward=forward, partner=partner, across=across, sides=sides, last=last, shard=shard)


def squares_flow(links, buf):
    tp = lax.axis_index("tp")
    xh, y = tp // 4, tp % 4

    def slot(dx, dy):
        return buf.at[(xh if dx == 0 else 1 - xh) * 4 + (y + dy) % 4]

    ring = [links.ticket() for _ in range(3)]
    cross = [links.ticket() for _ in range(4)]

    def own():
        links.start(ring[0], slot(0, 0), slot(0, 0), "yp")
        links.start(ring[1], slot(0, 0), slot(0, 0), "ym")
        links.start(cross[0], slot(0, 0), slot(0, 0), "xh")

    def all_():
        links.arrive(ring[0], slot(0, 3), "ym")
        links.start(ring[2], slot(0, 3), slot(0, 3), "yp")
        links.start(cross[3], slot(0, 3), slot(0, 3), "xh")
        links.arrive(ring[1], slot(0, 1), "yp")
        links.start(cross[1], slot(0, 1), slot(0, 1), "xh")
        links.arrive(ring[2], slot(0, 2), "ym")
        links.start(cross[2], slot(0, 2), slot(0, 2), "xh")
        for dy in range(4):
            links.arrive(cross[dy], slot(1, dy), "xh")

    return {"own": own, "all": all_}


def column_flow(links, buf, halves=2):
    ctx = lax.axis_index("ctx")
    z, xl, core = ctx // 4, (ctx // 2) % 2, ctx % 2
    rows = buf.shape[1]
    half = rows // 2

    def slot(dx, dz, dc=0, part=None):
        i = ((z + dz) % 4) * 4 + (xl if dx == 0 else 1 - xl) * 2 + (core if dc == 0 else 1 - core)
        ref = buf.at[i]
        return ref if part is None else ref.at[pl.ds(part * half, half)]

    T = {}
    for k in ("zp", "zm", "xl0", "xl1", "fa", "fb", "pzp0", "pzp1", "pzm0", "pzm1", "pfa", "pfb"):
        T[k] = links.ticket()
    for dx in range(2):
        for dz in range(4):
            T["co", dx, dz] = links.ticket()

    def share(dx, dz):
        links.start(T["co", dx, dz], slot(dx, dz), slot(dx, dz), "co")

    def own_x(part):
        links.start(T[f"xl{part}"], slot(0, 0, 0, part), slot(0, 0, 0, part), "xl")

    def own_z():
        links.start(T["zp"], slot(0, 0), slot(0, 0), "zp")
        links.start(T["zm"], slot(0, 0), slot(0, 0), "zm")
        share(0, 0)

    def forward():
        links.arrive(T["zp"], slot(0, 3), "zm")
        links.start(T["fa"], slot(0, 3, 0, 0), slot(0, 3, 0, 0), "zp")
        links.arrive(T["zm"], slot(0, 1), "zp")
        links.start(T["fb"], slot(0, 1, 0, 1), slot(0, 1, 0, 1), "zm")
        share(0, 3)
        share(0, 1)

    def partner(part):
        links.arrive(T[f"xl{part}"], slot(1, 0, 0, part), "xl")
        links.start(T[f"pzp{part}"], slot(1, 0, 0, part), slot(1, 0, 0, part), "zp")
        links.start(T[f"pzm{part}"], slot(1, 0, 0, part), slot(1, 0, 0, part), "zm")
        if part == 1:
            share(1, 0)

    def across():
        links.arrive(T["fa"], slot(0, 2, 0, 0), "zm")
        links.arrive(T["fb"], slot(0, 2, 0, 1), "zp")
        share(0, 2)

    def sides():
        links.arrive(T["pzp0"], slot(1, 3, 0, 0), "zm")
        links.start(T["pfa"], slot(1, 3, 0, 0), slot(1, 3, 0, 0), "zp")
        links.arrive(T["pzm0"], slot(1, 1, 0, 0), "zp")
        links.arrive(T["pzm1"], slot(1, 1, 0, 1), "zp")
        links.start(T["pfb"], slot(1, 1, 0, 1), slot(1, 1, 0, 1), "zm")
        links.arrive(T["pzp1"], slot(1, 3, 0, 1), "zm")
        share(1, 3)
        share(1, 1)

    def last():
        links.arrive(T["pfa"], slot(1, 2, 0, 0), "zm")
        links.arrive(T["pfb"], slot(1, 2, 0, 1), "zp")
        share(1, 2)

    def shared(pairs):
        for dx, dz in pairs:
            links.arrive(T["co", dx, dz], slot(dx, dz, 1), "co")

    everything = [(dx, dz) for dx in range(2) for dz in range(4)]
    return dict(own_x=own_x, own_z=own_z, forward=forward, partner=partner, across=across, sides=sides,
                last=last, shared=shared, everything=everything)


def project_kernel(tokens, wq, wk, wv, gain, cosine, sine, q_out, kv_out,
                   tbuf, wbuf, acc, squares, factors, send, recv, local):
    links = Links(send, recv)
    ctx, tp = lax.axis_index("ctx"), lax.axis_index("tp")
    qw, kw = wq.shape[1], wk.shape[1]
    width = qw + 2 * kw
    mine = [
        pltpu.make_async_copy(wq, wbuf.at[ctx, :, pl.ds(0, qw)], local.at[0]),
        pltpu.make_async_copy(wk, wbuf.at[ctx, :, pl.ds(qw, kw)], local.at[1]),
        pltpu.make_async_copy(wv, wbuf.at[ctx, :, pl.ds(qw + kw, kw)], local.at[2]),
        pltpu.make_async_copy(tokens, tbuf.at[pl.ds(tp * 2, 2)], local.at[3]),
    ]
    for c in mine:
        c.start()
    t = token_flow(links, tbuf, tokens)
    w = column_flow(links, wbuf)
    links.greet(("yp", "ym", "xh", "zp", "zm", "xl", "co"))
    for c in mine[:3]:
        c.wait()
    w["own_x"](0)
    t["own"](0)
    w["own_z"]()
    w["own_x"](1)
    t["own"](1)
    mine[3].wait()
    rows = tokens.shape[1]
    for s in range(2):
        wide = tbuf[tp * 2 + s].astype(jnp.float32)
        squares[tp, s] = lax.dot_general(
            jnp.ones((8, wide.shape[1]), jnp.float32), wide * wide, (((1,), (1,)), ((), ())),
            precision=lax.Precision.HIGHEST, preferred_element_type=jnp.float32,
        )
    acc[...] = jnp.zeros_like(acc)
    statistics = squares_flow(links, squares)
    statistics["own"]()

    t["forward"](0)
    w["forward"]()
    w["partner"](0)
    t["partner"](0)
    t["forward"](1)
    w["partner"](1)
    w["across"]()
    t["across"](0)
    t["partner"](1)
    t["across"](1)
    w["sides"]()
    t["sides"](0)
    w["last"]()
    w["shared"](w["everything"])
    statistics["all"]()
    features = 8 * tokens.shape[2]
    for s in range(2):
        total = squares[0, s]
        for i in range(1, 8):
            total = total + squares[i, s]
        factor = lax.rsqrt(total[:1] * (1.0 / features) + norm_eps)
        factors[s] = jnp.transpose(jnp.broadcast_to(factor, (128, rows)))

    def multiply(j, s):
        dx, dy = j // 4, j % 4
        shard = (tp // 4 + dx) % 2 * 4 + (tp % 4 + dy) % 4
        wide = tbuf[shard * 2 + s].astype(jnp.float32)
        x = (wide * factors[s, :, :1] * gain[shard]).astype(jnp.bfloat16)
        depth = x.shape[1]
        weights = wbuf[pl.ds(2 * shard, 2)].reshape(depth, width)
        acc[s] += jnp.dot(x, weights, preferred_element_type=jnp.float32)

    def run(js):
        first, count = js

        def body(i, _):
            multiply(first + i // 2, i % 2)
            return 0

        lax.fori_loop(0, 2 * count, body, 0)

    run((0, 5))
    t["sides"](1)
    run((5, 1))
    run((7, 1))
    t["last"](0)
    t["last"](1)
    run((6, 1))
    for s in range(2):
        c, d = cosine[s], sine[s]
        for h in range(width // HEAD_DIM):
            x = acc[s, :, h * HEAD_DIM:(h + 1) * HEAD_DIM]
            if h < width // HEAD_DIM - 1:
                x = x * c + pltpu.roll(x, HEAD_DIM // 2, 1) * d
            x = x.astype(jnp.bfloat16)
            if h < qw // HEAD_DIM:
                q_out[s, h] = x
            else:
                kv_out[h - qw // HEAD_DIM, s] = x
    links.finish()


def project(tokens, gain, cosine, sine, wq, wk, wv):
    n_ctx, n_tp = 16, 8
    seqs, rows, depth = tokens.shape
    width = wq.shape[1] + wk.shape[1] + wv.shape[1]
    bf16, f32 = jnp.bfloat16, jnp.float32
    heads = wq.shape[1] // HEAD_DIM
    anyspace = pl.BlockSpec(memory_space=pl.ANY)
    vmem = pl.BlockSpec(memory_space=pltpu.VMEM)
    return pl.pallas_call(
        project_kernel,
        out_shape=(
            jax.ShapeDtypeStruct((seqs, heads, rows, HEAD_DIM), bf16),
            jax.ShapeDtypeStruct((2, seqs, rows, HEAD_DIM), bf16),
        ),
        in_specs=[anyspace] * 4 + [vmem] * 3,
        out_specs=(vmem, vmem),
        scratch_shapes=[
            pltpu.VMEM((n_tp * seqs, rows, depth), bf16),
            pltpu.VMEM((n_ctx, wq.shape[0], width), bf16),
            pltpu.VMEM((seqs, rows, width), f32),
            pltpu.VMEM((n_tp, seqs, 8, rows), f32),
            pltpu.VMEM((seqs, rows, 128), f32),
            pltpu.SemaphoreType.DMA((44,)),
            pltpu.SemaphoreType.DMA((44,)),
            pltpu.SemaphoreType.DMA((4,)),
        ],
        compiler_params=pltpu.CompilerParams(
            collective_id=0, has_side_effects=True, vmem_limit_bytes=48 * 2**20
        ),
    )(tokens, wq, wk, wv, gain, cosine, sine)


def per_device(tokens, norm_gain, span_order, w_query, w_key, value_weight, w_out):
    sequence_batch, rows_dev, _ = tokens.shape
    head_size = HEAD_DIM
    query_heads = w_query.shape[1] // head_size
    key_heads = w_key.shape[1] // head_size
    group_width = query_heads // key_heads
    block_rows = rows_dev // 2
    total_rows = sequence_batch * rows_dev
    factor = 1.0 / math.sqrt(head_size)
    rank = lax.axis_index("ctx")
    query_pos = positions_of(span_order, rank * rows_dev, rows_dev, block_rows)
    latest = jnp.max(query_pos, axis=1)
    stat_shape = (sequence_batch, key_heads, group_width, rows_dev)
    initial = (
        jnp.full(stat_shape, masked_score, jnp.float32),
        jnp.zeros(stat_shape, jnp.float32),
        jnp.zeros(stat_shape + (head_size,), jnp.float32),
    )
    cosine, sine = angles(query_pos)
    query, kv = project(tokens, norm_gain.reshape(-1, 1, tokens.shape[2]), cosine, sine, w_query, w_key, value_weight)
    query = query.reshape(sequence_batch, key_heads, group_width, rows_dev, head_size)
    turned, own_values = kv[0][:, :, None], kv[1][:, :, None]
    key_piece, value_piece = in_one_piece((turned, own_values), "ctx", 1, 0)
    count = key_piece.shape[1]
    step_rows = 512

    def one_block(index, state):
        first = index * step_rows
        key_block = lax.dynamic_slice_in_dim(key_piece, first, step_rows, 1)
        value_block = lax.dynamic_slice_in_dim(value_piece, first, step_rows, 1)
        key_pos = positions_of(span_order, first, step_rows, block_rows)

        def update(current):
            peak, total, summed = current
            scores = (
                jnp.einsum(
                    "shgqd,skhd->shgqk", query, key_block, preferred_element_type=jnp.float32
                )
                * factor
            )
            allowed = key_pos[:, None, None, None, :] <= query_pos[:, None, None, :, None]
            scores = jnp.where(allowed, scores, masked_score)
            new_peak = jnp.maximum(peak, jnp.max(scores, axis=-1))
            weights = jnp.where(allowed, jnp.exp(scores - new_peak[..., None]), 0.0)
            shrink = jnp.exp(peak - new_peak)
            total = total * shrink + jnp.sum(weights, axis=-1)
            summed = summed * shrink[..., None] + jnp.einsum(
                "shgqk,skhd->shgqd",
                weights.astype(jnp.bfloat16),
                value_block,
                preferred_element_type=jnp.float32,
            )
            return (new_peak, total, summed)

        return lax.cond(
            jnp.all(jnp.min(key_pos, axis=1) > latest), lambda kept: kept, update, state
        )

    peak, total, summed = lax.fori_loop(0, count // step_rows, one_block, initial)
    attended = (summed / total[..., None]).astype(jnp.bfloat16)
    attended = attended.transpose(0, 3, 1, 2, 4).reshape(total_rows, query_heads * head_size)
    terms = jnp.dot(
        attended,
        lax.all_gather(w_out, "ctx", axis=1, tiled=True),
        preferred_element_type=jnp.float32,
    )
    mixed = lax.psum_scatter(terms.astype(jnp.bfloat16), "tp", scatter_dimension=1, tiled=True)
    return mixed.reshape(sequence_batch, rows_dev, mixed.shape[1])


def solution(mesh):
    placed = (
        P(None, "ctx", "tp"),
        P(),
        P(),
        P("ctx", "tp"),
        P("ctx", "tp"),
        P("ctx", "tp"),
        P("tp", "ctx"),
    )
    return jax.shard_map(
        per_device, mesh=mesh, in_specs=placed, out_specs=P(None, "ctx", "tp"), check_vma=False
    )
```

```python
import math

import jax
import jax.numpy as jnp
from jax import lax
from jax.experimental import pallas as pl
from jax.experimental.pallas import tpu as pltpu
from jax.sharding import PartitionSpec as P

HEAD_DIM = 128


theta_base = 500000.0
norm_eps = 1e-05
masked_score = -1e30


def in_one_piece(arrays, axis, dim, along):
    ends, at = ([], 0)
    for a in arrays[:-1]:
        at += a.shape[along]
        ends.append(at)
    both = jnp.concatenate(arrays, axis=along)
    return tuple(jnp.split(lax.all_gather(both, axis, axis=dim, tiled=True), ends, axis=along))


def angles(token_position):
    half = HEAD_DIM // 2
    freqs = jnp.exp(-(2.0 * jnp.arange(half, dtype=jnp.float32) / HEAD_DIM) * math.log(theta_base))
    angle = token_position.astype(jnp.float32)[..., None] * freqs
    cosine, sine = jnp.cos(angle), jnp.sin(angle)
    return jnp.concatenate([cosine, cosine], axis=-1), jnp.concatenate([-sine, sine], axis=-1)


MESH = pl.DeviceIdType.MESH


def neighbours():
    ctx, tp = lax.axis_index("ctx"), lax.axis_index("tp")
    z, xl, core = ctx // 4, (ctx // 2) % 2, ctx % 2
    xh, y = tp // 4, tp % 4

    def at(z_, xl_, core_, xh_, y_):
        return {"ctx": z_ * 4 + xl_ * 2 + core_, "tp": xh_ * 4 + y_}

    return {
        "yp": at(z, xl, core, xh, (y + 1) % 4),
        "ym": at(z, xl, core, xh, (y + 3) % 4),
        "y2": at(z, xl, core, xh, (y + 2) % 4),
        "xh": at(z, xl, core, 1 - xh, y),
        "xhyp": at(z, xl, core, 1 - xh, (y + 1) % 4),
        "xhym": at(z, xl, core, 1 - xh, (y + 3) % 4),
        "xhy2": at(z, xl, core, 1 - xh, (y + 2) % 4),
        "zp": at((z + 1) % 4, xl, core, xh, y),
        "zm": at((z + 3) % 4, xl, core, xh, y),
        "xl": at(z, 1 - xl, core, xh, y),
        "co": at(z, xl, 1 - core, xh, y),
    }


class Links:
    def __init__(self, send, recv):
        self.send, self.recv, self.count = send, recv, 0
        self.where = neighbours()
        self.sent = []

    def greet(self, names):
        barrier = pltpu.get_barrier_semaphore()
        for name in names:
            pl.semaphore_signal(barrier, 1, device_id=self.where[name], device_id_type=MESH)
        pl.semaphore_wait(barrier, len(names))

    def ticket(self):
        self.count += 1
        return self.count - 1

    def copy(self, ticket, src, dst, name):
        return pltpu.make_async_remote_copy(
            src, dst, self.send.at[ticket], self.recv.at[ticket],
            device_id=self.where[name], device_id_type=MESH,
        )

    def start(self, ticket, src, dst, name):
        c = self.copy(ticket, src, dst, name)
        c.start()
        self.sent.append(c)

    def arrive(self, ticket, here, name="co"):
        self.copy(ticket, here, here, name).wait_recv()

    def finish(self):
        for c in self.sent:
            c.wait_send()
        self.sent = []


def token_flow(links, tokens_buf, source):
    tp = lax.axis_index("tp")
    xh, y = tp // 4, tp % 4

    def shard(dx, dy):
        return (xh if dx == 0 else 1 - xh) * 4 + (y + dy) % 4

    def slot(dx, dy, s, rows=None):
        ref = tokens_buf.at[shard(dx, dy) * 2 + s]
        return ref if rows is None else ref.at[pl.ds(rows[0], rows[1])]

    rows = tokens_buf.shape[1]
    low, high = (0, rows // 2), (rows // 2, rows // 2)
    T = {}
    for s in range(2):
        for k in ("yp", "ym", "xh", "fa", "fb", "pyp", "pym", "x2"):
            T[k, s] = links.ticket()

    def own(s):
        links.start(T["xh", s], source.at[s], slot(0, 0, s), "xh")
        links.start(T["yp", s], source.at[s], slot(0, 0, s), "yp")
        links.start(T["ym", s], source.at[s], slot(0, 0, s), "ym")

    def forward(s):
        links.arrive(T["yp", s], slot(0, 3, s), "ym")
        links.start(T["fa", s], slot(0, 3, s, low), slot(0, 3, s, low), "yp")
        links.arrive(T["ym", s], slot(0, 1, s), "yp")
        links.start(T["fb", s], slot(0, 1, s, high), slot(0, 1, s, high), "ym")

    def partner(s):
        links.arrive(T["xh", s], slot(1, 0, s), "xh")
        links.start(T["pyp", s], slot(1, 0, s), slot(1, 0, s), "yp")
        links.start(T["pym", s], slot(1, 0, s), slot(1, 0, s), "ym")

    def across(s):
        links.arrive(T["fa", s], slot(0, 2, s, low), "ym")
        links.arrive(T["fb", s], slot(0, 2, s, high), "yp")
        links.start(T["x2", s], slot(0, 2, s), slot(0, 2, s), "xh")

    def sides(s):
        links.arrive(T["pyp", s], slot(1, 3, s), "ym")
        links.arrive(T["pym", s], slot(1, 1, s), "yp")

    def last(s):
        links.arrive(T["x2", s], slot(1, 2, s), "xh")

    return dict(own=own, forward=forward, partner=partner, across=across, sides=sides, last=last, shard=shard)


def squares_flow(links, buf):
    tp = lax.axis_index("tp")
    xh, y = tp // 4, tp % 4

    def slot(dx, dy):
        return buf.at[(xh if dx == 0 else 1 - xh) * 4 + (y + dy) % 4]

    routes = {"yp": (0, 3), "ym": (0, 1), "y2": (0, 2), "xh": (1, 0), "xhyp": (1, 3), "xhym": (1, 1), "xhy2": (1, 2)}
    T = {k: links.ticket() for k in routes}

    def own():
        for k in routes:
            links.start(T[k], slot(0, 0), slot(0, 0), k)

    def arrived():
        for k, where in routes.items():
            links.arrive(T[k], slot(*where))

    return {"own": own, "all": arrived}


def by_rank(z, xl, core):
    return z * 4 + xl * 2 + core


def by_pair(z, xl, core):
    return xl * 8 + z * 2 + core


def column_flow(links, buf, place=by_rank):
    ctx = lax.axis_index("ctx")
    z, xl, core = ctx // 4, (ctx // 2) % 2, ctx % 2
    rows = buf.shape[1]
    half = rows // 2

    def slot(dx, dz, dc=0, part=None):
        i = place((z + dz) % 4, xl if dx == 0 else 1 - xl, core if dc == 0 else 1 - core)
        ref = buf.at[i]
        return ref if part is None else ref.at[pl.ds(part * half, half)]

    T = {}
    for k in ("zp", "zm", "xl0", "xl1", "fa", "fb", "pzp0", "pzp1", "pzm0", "pzm1", "pfa", "pfb"):
        T[k] = links.ticket()
    for dx in range(2):
        for dz in range(4):
            T["co", dx, dz] = links.ticket()

    def share(dx, dz):
        links.start(T["co", dx, dz], slot(dx, dz), slot(dx, dz), "co")

    def own_x(part):
        links.start(T[f"xl{part}"], slot(0, 0, 0, part), slot(0, 0, 0, part), "xl")

    def own_z():
        links.start(T["zp"], slot(0, 0), slot(0, 0), "zp")
        links.start(T["zm"], slot(0, 0), slot(0, 0), "zm")
        share(0, 0)

    def forward():
        links.arrive(T["zp"], slot(0, 3), "zm")
        links.start(T["fa"], slot(0, 3, 0, 0), slot(0, 3, 0, 0), "zp")
        links.arrive(T["zm"], slot(0, 1), "zp")
        links.start(T["fb"], slot(0, 1, 0, 1), slot(0, 1, 0, 1), "zm")
        share(0, 3)
        share(0, 1)

    def partner(part):
        links.arrive(T[f"xl{part}"], slot(1, 0, 0, part), "xl")
        links.start(T[f"pzp{part}"], slot(1, 0, 0, part), slot(1, 0, 0, part), "zp")
        links.start(T[f"pzm{part}"], slot(1, 0, 0, part), slot(1, 0, 0, part), "zm")
        if part == 1:
            share(1, 0)

    def across():
        links.arrive(T["fa"], slot(0, 2, 0, 0), "zm")
        links.arrive(T["fb"], slot(0, 2, 0, 1), "zp")
        share(0, 2)

    def sides():
        links.arrive(T["pzp0"], slot(1, 3, 0, 0), "zm")
        links.start(T["pfa"], slot(1, 3, 0, 0), slot(1, 3, 0, 0), "zp")
        links.arrive(T["pzm0"], slot(1, 1, 0, 0), "zp")
        links.arrive(T["pzm1"], slot(1, 1, 0, 1), "zp")
        links.start(T["pfb"], slot(1, 1, 0, 1), slot(1, 1, 0, 1), "zm")
        links.arrive(T["pzp1"], slot(1, 3, 0, 1), "zm")
        share(1, 3)
        share(1, 1)

    def last():
        links.arrive(T["pfa"], slot(1, 2, 0, 0), "zm")
        links.arrive(T["pfb"], slot(1, 2, 0, 1), "zp")
        share(1, 2)

    def shared(pairs):
        for dx, dz in pairs:
            links.arrive(T["co", dx, dz], slot(dx, dz, 1), "co")

    everything = [(dx, dz) for dx in range(2) for dz in range(4)]
    return dict(own_x=own_x, own_z=own_z, forward=forward, partner=partner, across=across, sides=sides,
                last=last, shared=shared, everything=everything)


def attend(first_pair, pair, q_buf, kv_buf, query_pos, key_pos, peaks, sums, out):
    rows = q_buf.shape[1]
    heads = out.shape[2] // HEAD_DIM
    scale = math.log2(math.e) / math.sqrt(HEAD_DIM)

    def body(i, _):
        s, h = i // heads, i % heads
        at = pl.multiple_of(s * rows, rows)
        keys = kv_buf[pl.ds(pair * 8, 8), pl.ds(at, rows), :].reshape(8 * rows, HEAD_DIM)
        values = kv_buf[pl.ds(pair * 8, 8), pl.ds(2 * rows + at, rows), :].reshape(8 * rows, HEAD_DIM)
        scores = lax.dot_general(
            q_buf[i], keys, (((1,), (1,)), ((), ())), preferred_element_type=jnp.float32
        )
        allowed = key_pos[s * 2 + pair] <= query_pos[s, :, :1]
        scores = jnp.where(allowed, scores, masked_score)
        peak = jnp.maximum(jnp.max(scores, axis=1, keepdims=True), 1e-10 * masked_score)
        if not first_pair:
            before = peaks[i, :, :1]
            peak = jnp.maximum(peak, before)
        weights = jnp.exp2((scores - peak) * scale).astype(jnp.bfloat16)
        both = jnp.concatenate([values, jnp.ones_like(values)], axis=1)
        summed = jnp.dot(weights, both, preferred_element_type=jnp.float32)
        if first_pair:
            peaks[i] = jnp.broadcast_to(peak, peaks.shape[1:])
            sums[i] = summed
        else:
            summed = summed + sums[i] * jnp.exp2((before - peak) * scale)
            mean = summed[:, :HEAD_DIM] / summed[:, HEAD_DIM:]
            out[s, :, pl.ds(pl.multiple_of(h * HEAD_DIM, HEAD_DIM), HEAD_DIM)] = mean.astype(jnp.bfloat16)
        return 0

    lax.fori_loop(0, 2 * heads, body, 0)


def mix_kernel(tokens, wq, wk, wv, wo, gain, cosine, sine, query_pos, key_pos, mixed,
               tbuf, wbuf, acc, squares, factors, wobuf, kvbuf, qbuf, peaks, sums, attended,
               terms, from_x, from_y, halves, last_y, last_x, send, recv, local):
    links = Links(send, recv)
    ctx, tp = lax.axis_index("ctx"), lax.axis_index("tp")
    z, xl, core = ctx // 4, (ctx // 2) % 2, ctx % 2
    rows = tokens.shape[1]
    qw, kw = wq.shape[1], wk.shape[1]
    width = qw + 2 * kw
    heads = qw // HEAD_DIM
    mine = [
        pltpu.make_async_copy(wq, wbuf.at[ctx, :, pl.ds(0, qw)], local.at[0]),
        pltpu.make_async_copy(wk, wbuf.at[ctx, :, pl.ds(qw, kw)], local.at[1]),
        pltpu.make_async_copy(wv, wbuf.at[ctx, :, pl.ds(qw + kw, kw)], local.at[2]),
        pltpu.make_async_copy(tokens, tbuf.at[pl.ds(tp * 2, 2)], local.at[3]),
        pltpu.make_async_copy(wo, wobuf.at[ctx], local.at[4]),
    ]
    for c in (mine[3], *mine[:3], mine[4]):
        c.start()
    t = token_flow(links, tbuf, tokens)
    w = column_flow(links, wbuf)
    statistics = squares_flow(links, squares)
    o = column_flow(links, wobuf)
    kv = column_flow(links, kvbuf, by_pair)
    mine[3].wait()
    for s in range(2):
        wide = tbuf[tp * 2 + s].astype(jnp.float32)
        squares[tp, s] = lax.dot_general(
            jnp.ones((8, wide.shape[1]), jnp.float32), wide * wide, (((1,), (1,)), ((), ())),
            precision=lax.Precision.HIGHEST, preferred_element_type=jnp.float32,
        )
    for c in mine[:3]:
        c.wait()
    links.greet(("yp", "ym", "y2", "xh", "xhyp", "xhym", "xhy2", "zp", "zm", "xl", "co"))
    statistics["own"]()
    w["own_x"](0)
    t["own"](0)
    w["own_z"]()
    w["own_x"](1)
    t["own"](1)
    acc[...] = jnp.zeros_like(acc)
    mine[4].wait()

    t["forward"](0)
    w["forward"]()
    w["partner"](0)
    t["partner"](0)
    t["forward"](1)
    w["partner"](1)
    w["across"]()
    t["across"](0)
    t["partner"](1)
    t["across"](1)
    o["own_x"](0)
    o["own_x"](1)
    statistics["all"]()
    features = 8 * tokens.shape[2]
    for s in range(2):
        total = squares[0, s]
        for i in range(1, 8):
            total = total + squares[i, s]
        factor = lax.rsqrt(total[:1] * (1.0 / features) + norm_eps)
        factors[s] = jnp.transpose(jnp.broadcast_to(factor, (128, rows)))
    w["sides"]()
    o["own_z"]()
    t["sides"](0)
    w["last"]()
    w["shared"](w["everything"])

    def multiply(j, s):
        dx, dy = j // 4, j % 4
        shard = (tp // 4 + dx) % 2 * 4 + (tp % 4 + dy) % 4
        wide = tbuf[shard * 2 + s].astype(jnp.float32)
        x = (wide * factors[s, :, :1] * gain[shard]).astype(jnp.bfloat16)
        weights = wbuf[pl.ds(2 * shard, 2)].reshape(x.shape[1], width)
        acc[s] += jnp.dot(x, weights, preferred_element_type=jnp.float32)

    def run(first, count):
        def body(i, _):
            multiply(first + i // 2, i % 2)
            return 0

        lax.fori_loop(0, 2 * count, body, 0)

    run(0, 5)
    o["forward"]()
    t["sides"](1)
    run(5, 1)
    run(7, 1)
    o["across"]()
    t["last"](0)
    t["last"](1)
    run(6, 1)

    own = by_pair(z, xl, core)

    def turn(x, s):
        return x * cosine[s] + pltpu.roll(x, HEAD_DIM // 2, 1) * sine[s]

    for s in range(2):
        kvbuf[own, s * rows:(s + 1) * rows] = turn(acc[s, :, qw:qw + kw], s).astype(jnp.bfloat16)
        kvbuf[own, (2 + s) * rows:(3 + s) * rows] = acc[s, :, qw + kw:].astype(jnp.bfloat16)
    kv["own_x"](0)
    kv["own_z"]()
    kv["own_x"](1)
    for s in range(2):
        for h in range(heads):
            qbuf[s * heads + h] = turn(acc[s, :, h * HEAD_DIM:(h + 1) * HEAD_DIM], s).astype(jnp.bfloat16)
    kv["partner"](0)
    kv["forward"]()
    kv["partner"](1)
    kv["across"]()
    kv["shared"]([(0, dz) for dz in range(4)])
    kv["sides"]()
    o["partner"](0)
    o["partner"](1)
    attend(True, xl, qbuf, kvbuf, query_pos, key_pos, peaks, sums, attended)
    kv["last"]()
    kv["shared"]([(1, dz) for dz in range(4)])
    o["sides"]()
    attend(False, 1 - xl, qbuf, kvbuf, query_pos, key_pos, peaks, sums, attended)
    o["last"]()
    o["shared"](o["everything"])

    half = terms.shape[2]

    def term(dx, dy, c):
        return (dx * 4 + dy) * 2 + c

    def products(first, count):
        def body(i, _):
            rel, c = first + i // 2, i % 2
            block = (tp // 4 + rel // 4) % 2 * 4 + (tp % 4 + rel % 4) % 4
            terms[2 * first + i] = jnp.dot(
                attended[...].reshape(2 * rows, qw), wobuf[2 * block + c], preferred_element_type=jnp.float32
            ).astype(jnp.bfloat16)
            return 0

        lax.fori_loop(0, 2 * count, body, 0)

    R = {}
    for k in ("x", "yp", "ym", "h", "zyp", "zym", "zx"):
        for c in range(2):
            R[k, c] = links.ticket()

    def add(index, *others):
        total = terms[index].astype(jnp.float32)
        for ref in others:
            total = total + ref[...].astype(jnp.float32)
        return total

    products(6, 1)
    for c in range(2):
        links.start(R["x", c], terms.at[term(1, 2, c)], from_x.at[c], "xh")
    products(5, 1)
    for c in range(2):
        links.start(R["yp", c], terms.at[term(1, 1, c)], from_y.at[c], "yp")
    products(7, 1)
    for c in range(2):
        links.start(R["ym", c], terms.at[term(1, 3, c)], from_y.at[2 + c], "ym")
    products(0, 5)
    for c, to in ((0, "yp"), (1, "ym")):
        links.arrive(R["x", c], from_x.at[c])
        terms[term(0, 2, c)] = add(term(0, 2, c), from_x.at[c]).astype(jnp.bfloat16)
        links.start(R["h", c], terms.at[term(0, 2, c)], halves.at[c], to)
    links.start(R["zyp", 1], terms.at[term(0, 1, 1)], last_y.at[1], "yp")
    links.start(R["zym", 0], terms.at[term(0, 3, 0)], last_y.at[2], "ym")
    for c in range(2):
        links.arrive(R["yp", c], from_y.at[c])
        links.arrive(R["ym", c], from_y.at[2 + c])
        terms[term(1, 0, c)] = add(term(1, 0, c), from_y.at[c], from_y.at[2 + c]).astype(jnp.bfloat16)
        links.start(R["zx", c], terms.at[term(1, 0, c)], last_x.at[c], "xh")
    links.arrive(R["h", 0], halves.at[0])
    terms[term(0, 1, 0)] = add(term(0, 1, 0), halves.at[0]).astype(jnp.bfloat16)
    links.start(R["zyp", 0], terms.at[term(0, 1, 0)], last_y.at[0], "yp")
    links.arrive(R["h", 1], halves.at[1])
    terms[term(0, 3, 1)] = add(term(0, 3, 1), halves.at[1]).astype(jnp.bfloat16)
    links.start(R["zym", 1], terms.at[term(0, 3, 1)], last_y.at[3], "ym")
    for c in range(2):
        links.arrive(R["zx", c], last_x.at[c])
        links.arrive(R["zyp", c], last_y.at[c])
        links.arrive(R["zym", c], last_y.at[2 + c])
        total = add(term(0, 0, c), last_x.at[c], last_y.at[c], last_y.at[2 + c])
        mixed[:, :, c * half:(c + 1) * half] = total.astype(jnp.bfloat16).reshape(2, rows, half)
    links.finish()


def per_device(tokens, norm_gain, span_order, w_query, w_key, value_weight, w_out):
    n_ctx, n_tp = 16, 8
    seqs, rows, depth = tokens.shape
    qw = w_query.shape[1]
    width = qw + w_key.shape[1] + value_weight.shape[1]
    heads = qw // HEAD_DIM
    blocks = span_order.shape[1]
    block_rows = n_ctx * rows // blocks
    bf16, f32 = jnp.bfloat16, jnp.float32
    position = (span_order[:, :, None] * block_rows + jnp.arange(block_rows, dtype=jnp.int32)).reshape(seqs, n_ctx * rows)
    query_pos = lax.dynamic_slice_in_dim(position, lax.axis_index("ctx") * rows, rows, 1)
    cosine, sine = angles(query_pos)
    key_pos = position.reshape(seqs, 4, 2, 2 * rows).transpose(0, 2, 1, 3).reshape(2 * seqs, 1, 8 * rows)
    query_pos = jnp.broadcast_to(query_pos[:, :, None], (seqs, rows, 128))
    anyspace = pl.BlockSpec(memory_space=pl.ANY)
    vmem = pl.BlockSpec(memory_space=pltpu.VMEM)
    half = depth // 2
    return pl.pallas_call(
        mix_kernel,
        out_shape=jax.ShapeDtypeStruct(tokens.shape, bf16),
        in_specs=[anyspace] * 5 + [vmem] * 5,
        out_specs=vmem,
        scratch_shapes=[
            pltpu.VMEM((n_tp * seqs, rows, depth), bf16),
            pltpu.VMEM((n_ctx, w_query.shape[0], width), bf16),
            pltpu.VMEM((seqs, rows, width), f32),
            pltpu.VMEM((n_tp, seqs, 8, rows), f32),
            pltpu.VMEM((seqs, rows, 128), f32),
            pltpu.VMEM((n_ctx, *w_out.shape), bf16),
            pltpu.VMEM((n_ctx, 2 * seqs * rows, HEAD_DIM), bf16),
            pltpu.VMEM((seqs * heads, rows, HEAD_DIM), bf16),
            pltpu.VMEM((seqs * heads, rows, 128), f32),
            pltpu.VMEM((seqs * heads, rows, 2 * HEAD_DIM), f32),
            pltpu.VMEM((seqs, rows, qw), bf16),
            pltpu.VMEM((2 * n_tp, seqs * rows, half), bf16),
            pltpu.VMEM((2, seqs * rows, half), bf16),
            pltpu.VMEM((4, seqs * rows, half), bf16),
            pltpu.VMEM((2, seqs * rows, half), bf16),
            pltpu.VMEM((4, seqs * rows, half), bf16),
            pltpu.VMEM((2, seqs * rows, half), bf16),
            pltpu.SemaphoreType.DMA((104,)),
            pltpu.SemaphoreType.DMA((104,)),
            pltpu.SemaphoreType.DMA((5,)),
        ],
        compiler_params=pltpu.CompilerParams(
            collective_id=0, has_side_effects=True, vmem_limit_bytes=63 * 2**20
        ),
    )(tokens, w_query, w_key, value_weight, w_out, norm_gain.reshape(n_tp, 1, depth), cosine, sine, query_pos, key_pos)


def solution(mesh):
    placed = (
        P(None, "ctx", "tp"),
        P(),
        P(),
        P("ctx", "tp"),
        P("ctx", "tp"),
        P("ctx", "tp"),
        P("tp", "ctx"),
    )
    return jax.shard_map(
        per_device, mesh=mesh, in_specs=placed, out_specs=P(None, "ctx", "tp"), check_vma=False
    )
```

```python
import math

import jax
import jax.numpy as jnp
from jax import lax
from jax.experimental import pallas as pl
from jax.experimental.pallas import tpu as pltpu
from jax.sharding import PartitionSpec as P

HEAD_DIM = 128


theta_base = 500000.0
norm_eps = 1e-05
masked_score = -1e30


def in_one_piece(arrays, axis, dim, along):
    ends, at = ([], 0)
    for a in arrays[:-1]:
        at += a.shape[along]
        ends.append(at)
    both = jnp.concatenate(arrays, axis=along)
    return tuple(jnp.split(lax.all_gather(both, axis, axis=dim, tiled=True), ends, axis=along))


def angles(token_position):
    half = HEAD_DIM // 2
    freqs = jnp.exp(-(2.0 * jnp.arange(half, dtype=jnp.float32) / HEAD_DIM) * math.log(theta_base))
    angle = token_position.astype(jnp.float32)[..., None] * freqs
    cosine, sine = jnp.cos(angle), jnp.sin(angle)
    return jnp.concatenate([cosine, cosine], axis=-1), jnp.concatenate([-sine, sine], axis=-1)


MESH = pl.DeviceIdType.MESH


def neighbours():
    ctx, tp = lax.axis_index("ctx"), lax.axis_index("tp")
    z, xl, core = ctx // 4, (ctx // 2) % 2, ctx % 2
    xh, y = tp // 4, tp % 4

    def at(z_, xl_, core_, xh_, y_):
        return {"ctx": z_ * 4 + xl_ * 2 + core_, "tp": xh_ * 4 + y_}

    return {
        "yp": at(z, xl, core, xh, (y + 1) % 4),
        "ym": at(z, xl, core, xh, (y + 3) % 4),
        "y2": at(z, xl, core, xh, (y + 2) % 4),
        "xh": at(z, xl, core, 1 - xh, y),
        "xhyp": at(z, xl, core, 1 - xh, (y + 1) % 4),
        "xhym": at(z, xl, core, 1 - xh, (y + 3) % 4),
        "xhy2": at(z, xl, core, 1 - xh, (y + 2) % 4),
        "zp": at((z + 1) % 4, xl, core, xh, y),
        "zm": at((z + 3) % 4, xl, core, xh, y),
        "xl": at(z, 1 - xl, core, xh, y),
        "co": at(z, xl, 1 - core, xh, y),
    }


class Links:
    def __init__(self, send, recv):
        self.send, self.recv, self.count = send, recv, 0
        self.where = neighbours()
        self.sent = []

    def greet(self, names):
        barrier = pltpu.get_barrier_semaphore()
        for name in names:
            pl.semaphore_signal(barrier, 1, device_id=self.where[name], device_id_type=MESH)
        pl.semaphore_wait(barrier, len(names))

    def ticket(self):
        self.count += 1
        return self.count - 1

    def copy(self, ticket, src, dst, name):
        return pltpu.make_async_remote_copy(
            src, dst, self.send.at[ticket], self.recv.at[ticket],
            device_id=self.where[name], device_id_type=MESH,
        )

    def start(self, ticket, src, dst, name):
        c = self.copy(ticket, src, dst, name)
        c.start()
        self.sent.append(c)

    def arrive(self, ticket, here, name="co"):
        self.copy(ticket, here, here, name).wait_recv()

    def finish(self):
        for c in self.sent:
            c.wait_send()
        self.sent = []


def token_flow(links, tokens_buf, source):
    tp = lax.axis_index("tp")
    xh, y = tp // 4, tp % 4

    def shard(dx, dy):
        return (xh if dx == 0 else 1 - xh) * 4 + (y + dy) % 4

    def slot(dx, dy, s, rows=None):
        ref = tokens_buf.at[shard(dx, dy) * 2 + s]
        return ref if rows is None else ref.at[pl.ds(rows[0], rows[1])]

    rows = tokens_buf.shape[1]
    low, high = (0, rows // 2), (rows // 2, rows // 2)
    T = {}
    for s in range(2):
        for k in ("yp", "ym", "xh", "fa", "fb", "pyp", "pym", "x2"):
            T[k, s] = links.ticket()
    T["pfa"], T["pfb"] = links.ticket(), links.ticket()

    def own(s, first):
        if not first:
            links.start(T["xh", s], source.at[s], slot(0, 0, s), "xh")
            return
        links.start(T["yp", s], source.at[s], slot(0, 0, s), "yp")
        links.start(T["ym", s], source.at[s], slot(0, 0, s), "ym")

    def forward(s):
        links.arrive(T["yp", s], slot(0, 3, s), "ym")
        links.start(T["fa", s], slot(0, 3, s, low), slot(0, 3, s, low), "yp")
        links.arrive(T["ym", s], slot(0, 1, s), "yp")
        links.start(T["fb", s], slot(0, 1, s, high), slot(0, 1, s, high), "ym")

    def partner(s):
        links.arrive(T["xh", s], slot(1, 0, s), "xh")
        links.start(T["pyp", s], slot(1, 0, s), slot(1, 0, s), "yp")
        links.start(T["pym", s], slot(1, 0, s), slot(1, 0, s), "ym")

    def across(s):
        links.arrive(T["fa", s], slot(0, 2, s, low), "ym")
        links.arrive(T["fb", s], slot(0, 2, s, high), "yp")
        if s == 0:
            links.start(T["x2", s], slot(0, 2, s), slot(0, 2, s), "xh")

    def sides(s):
        links.arrive(T["pyp", s], slot(1, 3, s), "ym")
        if s == 1:
            links.start(T["pfa"], slot(1, 3, s, low), slot(1, 3, s, low), "yp")
        links.arrive(T["pym", s], slot(1, 1, s), "yp")
        if s == 1:
            links.start(T["pfb"], slot(1, 1, s, high), slot(1, 1, s, high), "ym")

    def last(s):
        if s == 0:
            links.arrive(T["x2", s], slot(1, 2, s), "xh")
        else:
            links.arrive(T["pfa"], slot(1, 2, s, low), "ym")
            links.arrive(T["pfb"], slot(1, 2, s, high), "yp")

    return dict(own=own, forward=forward, partner=partner, across=across, sides=sides, last=last, shard=shard)


def squares_flow(links, buf):
    tp = lax.axis_index("tp")
    xh, y = tp // 4, tp % 4

    def slot(dx, dy):
        return buf.at[(xh if dx == 0 else 1 - xh) * 4 + (y + dy) % 4]

    routes = {"yp": (0, 3), "ym": (0, 1), "y2": (0, 2), "xh": (1, 0), "xhyp": (1, 3), "xhym": (1, 1), "xhy2": (1, 2)}
    T = {k: links.ticket() for k in routes}

    def own():
        for k in routes:
            links.start(T[k], slot(0, 0), slot(0, 0), k)

    def arrived():
        for k, where in routes.items():
            links.arrive(T[k], slot(*where))

    return {"own": own, "all": arrived}


def by_rank(z, xl, core):
    return z * 4 + xl * 2 + core


def by_pair(z, xl, core):
    return xl * 8 + z * 2 + core


def column_flow(links, buf, place=by_rank, far_by_x=False):
    ctx = lax.axis_index("ctx")
    z, xl, core = ctx // 4, (ctx // 2) % 2, ctx % 2
    rows = buf.shape[1]
    half = rows // 2

    def slot(dx, dz, dc=0, part=None):
        i = place((z + dz) % 4, xl if dx == 0 else 1 - xl, core if dc == 0 else 1 - core)
        ref = buf.at[i]
        return ref if part is None else ref.at[pl.ds(part * half, half)]

    T = {}
    for k in ("zp", "zm", "xl0", "xl1", "fa", "fb", "pzp0", "pzp1", "pzm0", "pzm1", "pfa", "pfb", "x2"):
        T[k] = links.ticket()
    for dx in range(2):
        for dz in range(4):
            T["co", dx, dz] = links.ticket()

    def share(dx, dz):
        links.start(T["co", dx, dz], slot(dx, dz), slot(dx, dz), "co")

    def own_x(part):
        links.start(T[f"xl{part}"], slot(0, 0, 0, part), slot(0, 0, 0, part), "xl")

    def own_z():
        links.start(T["zp"], slot(0, 0), slot(0, 0), "zp")
        links.start(T["zm"], slot(0, 0), slot(0, 0), "zm")
        share(0, 0)

    def forward():
        links.arrive(T["zp"], slot(0, 3), "zm")
        links.start(T["fa"], slot(0, 3, 0, 0), slot(0, 3, 0, 0), "zp")
        links.arrive(T["zm"], slot(0, 1), "zp")
        links.start(T["fb"], slot(0, 1, 0, 1), slot(0, 1, 0, 1), "zm")
        share(0, 3)
        share(0, 1)

    def partner(part):
        links.arrive(T[f"xl{part}"], slot(1, 0, 0, part), "xl")
        links.start(T[f"pzp{part}"], slot(1, 0, 0, part), slot(1, 0, 0, part), "zp")
        links.start(T[f"pzm{part}"], slot(1, 0, 0, part), slot(1, 0, 0, part), "zm")
        if part == 1:
            share(1, 0)

    def across():
        links.arrive(T["fa"], slot(0, 2, 0, 0), "zm")
        links.arrive(T["fb"], slot(0, 2, 0, 1), "zp")
        if far_by_x:
            links.start(T["x2"], slot(0, 2), slot(0, 2), "xl")
        share(0, 2)

    def sides():
        if far_by_x:
            for part in range(2):
                links.arrive(T[f"pzp{part}"], slot(1, 3, 0, part), "zm")
                links.arrive(T[f"pzm{part}"], slot(1, 1, 0, part), "zp")
            share(1, 3)
            share(1, 1)
            return
        links.arrive(T["pzp0"], slot(1, 3, 0, 0), "zm")
        links.start(T["pfa"], slot(1, 3, 0, 0), slot(1, 3, 0, 0), "zp")
        links.arrive(T["pzm0"], slot(1, 1, 0, 0), "zp")
        links.arrive(T["pzm1"], slot(1, 1, 0, 1), "zp")
        links.start(T["pfb"], slot(1, 1, 0, 1), slot(1, 1, 0, 1), "zm")
        links.arrive(T["pzp1"], slot(1, 3, 0, 1), "zm")
        share(1, 3)
        share(1, 1)

    def last():
        if far_by_x:
            links.arrive(T["x2"], slot(1, 2), "xl")
            share(1, 2)
            return
        links.arrive(T["pfa"], slot(1, 2, 0, 0), "zm")
        links.arrive(T["pfb"], slot(1, 2, 0, 1), "zp")
        share(1, 2)

    def shared(pairs):
        for dx, dz in pairs:
            links.arrive(T["co", dx, dz], slot(dx, dz, 1), "co")

    everything = [(dx, dz) for dx in range(2) for dz in range(4)]
    return dict(own_x=own_x, own_z=own_z, forward=forward, partner=partner, across=across, sides=sides,
                last=last, shared=shared, everything=everything)


def attend(s, first_pair, pair, q_buf, kv_buf, query_pos, key_pos, peaks, sums, out):
    rows = q_buf.shape[1]
    heads = out.shape[2] // HEAD_DIM
    scale = math.log2(math.e) / math.sqrt(HEAD_DIM)

    def body(h, _):
        i = s * heads + h
        held = pl.ds(s * 16 + pair * 8, 8)
        keys = kv_buf[held, :rows, :].reshape(8 * rows, HEAD_DIM)
        values = kv_buf[held, rows:, :].reshape(8 * rows, HEAD_DIM)
        scores = lax.dot_general(
            q_buf[i], keys, (((1,), (1,)), ((), ())), preferred_element_type=jnp.float32
        )
        allowed = key_pos[s * 2 + pair] <= query_pos[s, :, :1]
        scores = jnp.where(allowed, scores, masked_score)
        peak = jnp.maximum(jnp.max(scores, axis=1, keepdims=True), 1e-10 * masked_score)
        if not first_pair:
            before = peaks[h, :, :1]
            peak = jnp.maximum(peak, before)
        weights = jnp.exp2((scores - peak) * scale).astype(jnp.bfloat16)
        both = jnp.concatenate([values, jnp.ones_like(values)], axis=1)
        summed = jnp.dot(weights, both, preferred_element_type=jnp.float32)
        if first_pair:
            peaks[h] = jnp.broadcast_to(peak, peaks.shape[1:])
            sums[h] = summed
        else:
            summed = summed + sums[h] * jnp.exp2((before - peak) * scale)
            mean = summed[:, :HEAD_DIM] / summed[:, HEAD_DIM:]
            out[s, :, pl.ds(pl.multiple_of(h * HEAD_DIM, HEAD_DIM), HEAD_DIM)] = mean.astype(jnp.bfloat16)
        return 0

    lax.fori_loop(0, heads, body, 0)


def mix_kernel(tokens, wq, wk, wv, wo, gain, cosine, sine, query_pos, key_pos, mixed,
               tbuf, wbuf, acc, squares, factors, wobuf, kvbuf, qbuf, peaks, sums, attended,
               terms, from_x, from_y, halves, last_y, last_x, send, recv, local):
    links = Links(send, recv)
    ctx, tp = lax.axis_index("ctx"), lax.axis_index("tp")
    z, xl, core = ctx // 4, (ctx // 2) % 2, ctx % 2
    rows = tokens.shape[1]
    qw, kw = wq.shape[1], wk.shape[1]
    width = qw + 2 * kw
    heads = qw // HEAD_DIM
    mine = [
        pltpu.make_async_copy(tokens, tbuf.at[pl.ds(tp * 2, 2)], local.at[3]),
        pltpu.make_async_copy(wq, wbuf.at[ctx, :, pl.ds(0, qw)], local.at[0]),
        pltpu.make_async_copy(wk, wbuf.at[ctx, :, pl.ds(qw, kw)], local.at[1]),
        pltpu.make_async_copy(wv, wbuf.at[ctx, :, pl.ds(qw + kw, kw)], local.at[2]),
        pltpu.make_async_copy(wo, wobuf.at[ctx], local.at[4]),
    ]
    for c in mine:
        c.start()
    t = token_flow(links, tbuf, tokens)
    w = column_flow(links, wbuf)
    statistics = squares_flow(links, squares)
    o = column_flow(links, wobuf, far_by_x=True)
    kv = [
        column_flow(links, kvbuf, lambda z_, xl_, core_, s=s: s * 16 + by_pair(z_, xl_, core_), far_by_x=True)
        for s in range(2)
    ]
    links.greet(("yp", "ym", "y2", "xh", "xhyp", "xhym", "xhy2", "zp", "zm", "xl", "co"))
    t["own"](0, first=True)
    for c in mine[1:4]:
        c.wait()
    w["own_x"](0)
    w["own_z"]()
    t["own"](1, first=False)
    w["own_x"](1)
    t["own"](1, first=True)
    t["own"](0, first=False)
    mine[0].wait()
    for s in range(2):
        wide = tbuf[tp * 2 + s].astype(jnp.float32)
        squares[tp, s] = lax.dot_general(
            jnp.ones((8, wide.shape[1]), jnp.float32), wide * wide, (((1,), (1,)), ((), ())),
            precision=lax.Precision.HIGHEST, preferred_element_type=jnp.float32,
        )
    statistics["own"]()
    acc[...] = jnp.zeros_like(acc)
    mine[4].wait()

    def multiply(shard):
        wide = tbuf[pl.ds(shard * 2, 2)].astype(jnp.float32).reshape(2 * rows, tokens.shape[2])
        x = (wide * factors[:, :1] * gain[shard]).astype(jnp.bfloat16)
        weights = wbuf[pl.ds(2 * shard, 2)].reshape(x.shape[1], width)
        acc[...] += jnp.dot(x, weights, preferred_element_type=jnp.float32)

    def run(dx, first, count, stride=1):
        def body(i, _):
            multiply((tp // 4 + dx) % 2 * 4 + (tp % 4 + first + stride * i) % 4)
            return 0

        lax.fori_loop(0, count, body, 0)

    own_column, other_column = [[(dx, dz) for dz in range(4)] for dx in range(2)]
    near = (xl + tp % 4) % 2
    t["forward"](0)
    w["partner"](0)
    w["forward"]()
    t["forward"](1)
    t["partner"](1)
    w["across"]()
    w["partner"](1)
    t["across"](0)
    t["across"](1)
    o["own_x"](0)
    o["own_x"](1)
    statistics["all"]()
    features = 8 * tokens.shape[2]
    for s in range(2):
        total = squares[0, s]
        for i in range(1, 8):
            total = total + squares[i, s]
        factor = lax.rsqrt(total[:1] * (1.0 / features) + norm_eps)
        factors[s * rows:(s + 1) * rows] = jnp.transpose(jnp.broadcast_to(factor, (128, rows)))
    w["shared"](own_column)
    t["partner"](0)
    run(0, near, 2, 2)
    w["sides"]()
    o["own_z"]()
    t["sides"](1)
    w["last"]()
    w["shared"](other_column)
    run(0, 1 - near, 2, 2)
    run(1, 0, 1)
    t["sides"](0)
    run(1, 1, 2, 2)
    t["last"](0)
    t["last"](1)
    o["forward"]()
    run(1, 2, 1)

    own = by_pair(z, xl, core)

    def turn(x, s):
        return x * cosine[s] + pltpu.roll(x, HEAD_DIM // 2, 1) * sine[s]

    for s in range(2):
        at = pl.ds(s * rows, rows)
        kvbuf[s * 16 + own, :rows] = turn(acc[at, qw:qw + kw], s).astype(jnp.bfloat16)
        kvbuf[s * 16 + own, rows:] = acc[at, qw + kw:].astype(jnp.bfloat16)
    for s in range(2):
        kv[s]["own_x"](0)
        kv[s]["own_z"]()
        kv[s]["own_x"](1)
    for s in range(2):
        for h in range(heads):
            qbuf[s * heads + h] = turn(acc[pl.ds(s * rows, rows), h * HEAD_DIM:(h + 1) * HEAD_DIM], s).astype(jnp.bfloat16)

    def look(s, first_pair):
        attend(s, first_pair, xl if first_pair else 1 - xl, qbuf, kvbuf, query_pos, key_pos, peaks, sums, attended)

    half = mixed.shape[2] // 2
    cut = [pl.ds(0, half), pl.ds(half, half)]

    def term(dx, dy, s):
        return (dx * 4 + dy) * 2 + s

    def products(s, first, count):
        def body(i, _):
            rel = first + i
            block = (tp // 4 + rel // 4) % 2 * 4 + (tp % 4 + rel % 4) % 4
            for c in range(2):
                terms[rel * 2 + s, :, c * half:(c + 1) * half] = jnp.dot(
                    attended[s], wobuf[2 * block + c], preferred_element_type=jnp.float32
                ).astype(jnp.bfloat16)
            return 0

        lax.fori_loop(0, count, body, 0)

    R = {(k, s): links.ticket() for s in range(2) for k in ("x", "yp", "ym", "h0", "h1", "zyp0", "zyp1", "zym0", "zym1", "zx")}

    def wide(ref):
        return ref[...].astype(jnp.float32)

    def open_sums(s):
        products(s, 6, 1)
        links.start(R["x", s], terms.at[term(1, 2, s)], from_x.at[s], "xh")
        products(s, 5, 1)
        links.start(R["yp", s], terms.at[term(1, 1, s)], from_y.at[s], "yp")
        products(s, 7, 1)
        links.start(R["ym", s], terms.at[term(1, 3, s)], from_y.at[2 + s], "ym")
        products(s, 0, 5)

    def far(s):
        links.arrive(R["x", s], from_x.at[s])
        here = terms.at[term(0, 2, s)]
        here[...] = (wide(here) + wide(from_x.at[s])).astype(jnp.bfloat16)
        for c, to in ((0, "yp"), (1, "ym")):
            links.start(R[f"h{c}", s], here.at[:, cut[c]], halves.at[2 * c + s], to)
        links.start(R["zyp1", s], terms.at[term(0, 1, s), :, cut[1]], last_y.at[s, :, cut[1]], "yp")
        links.start(R["zym0", s], terms.at[term(0, 3, s), :, cut[0]], last_y.at[2 + s, :, cut[0]], "ym")

    def over(s):
        links.arrive(R["yp", s], from_y.at[s])
        links.arrive(R["ym", s], from_y.at[2 + s])
        here = terms.at[term(1, 0, s)]
        here[...] = (wide(here) + wide(from_y.at[s]) + wide(from_y.at[2 + s])).astype(jnp.bfloat16)
        links.start(R["zx", s], here, last_x.at[s], "xh")

    def close(s):
        for c, dy, k, to in ((0, 1, "zyp0", "yp"), (1, 3, "zym1", "ym")):
            links.arrive(R[f"h{c}", s], halves.at[2 * c + s])
            here = terms.at[term(0, dy, s), :, cut[c]]
            here[...] = (wide(here) + wide(halves.at[2 * c + s])).astype(jnp.bfloat16)
            links.start(R[k, s], here, last_y.at[2 * c + s, :, cut[c]], to)

    def result(s):
        links.arrive(R["zx", s], last_x.at[s])
        for c in range(2):
            links.arrive(R[f"zyp{c}", s], last_y.at[s, :, cut[c]])
            links.arrive(R[f"zym{c}", s], last_y.at[2 + s, :, cut[c]])
        total = wide(terms.at[term(0, 0, s)]) + wide(last_x.at[s]) + wide(last_y.at[s]) + wide(last_y.at[2 + s])
        mixed[s] = total.astype(jnp.bfloat16)

    for s in range(2):
        kv[s]["partner"](0)
        kv[s]["forward"]()
        kv[s]["partner"](1)
    o["partner"](0)
    o["partner"](1)
    for s in range(2):
        kv[s]["across"]()
    o["across"]()
    kv[0]["shared"](own_column)
    look(0, True)
    kv[0]["sides"]()
    kv[1]["sides"]()
    kv[0]["last"]()
    kv[1]["last"]()
    kv[0]["shared"](other_column)
    look(0, False)
    o["sides"]()
    o["last"]()
    o["shared"](own_column + other_column)
    open_sums(0)
    kv[1]["shared"](own_column)
    look(1, True)
    far(0)
    over(0)
    kv[1]["shared"](other_column)
    look(1, False)
    open_sums(1)
    close(0)
    far(1)
    over(1)
    close(1)
    result(0)
    result(1)
    links.finish()


def per_device(tokens, norm_gain, span_order, w_query, w_key, value_weight, w_out):
    n_ctx, n_tp = 16, 8
    seqs, rows, depth = tokens.shape
    qw = w_query.shape[1]
    width = qw + w_key.shape[1] + value_weight.shape[1]
    heads = qw // HEAD_DIM
    blocks = span_order.shape[1]
    block_rows = n_ctx * rows // blocks
    bf16, f32 = jnp.bfloat16, jnp.float32
    position = (span_order[:, :, None] * block_rows + jnp.arange(block_rows, dtype=jnp.int32)).reshape(seqs, n_ctx * rows)
    query_pos = lax.dynamic_slice_in_dim(position, lax.axis_index("ctx") * rows, rows, 1)
    cosine, sine = angles(query_pos)
    key_pos = position.reshape(seqs, 4, 2, 2 * rows).transpose(0, 2, 1, 3).reshape(2 * seqs, 1, 8 * rows)
    query_pos = jnp.broadcast_to(query_pos[:, :, None], (seqs, rows, 128))
    anyspace = pl.BlockSpec(memory_space=pl.ANY)
    vmem = pl.BlockSpec(memory_space=pltpu.VMEM)
    return pl.pallas_call(
        mix_kernel,
        out_shape=jax.ShapeDtypeStruct(tokens.shape, bf16),
        in_specs=[anyspace] * 5 + [vmem] * 5,
        out_specs=vmem,
        scratch_shapes=[
            pltpu.VMEM((n_tp * seqs, rows, depth), bf16),
            pltpu.VMEM((n_ctx, w_query.shape[0], width), bf16),
            pltpu.VMEM((seqs * rows, width), f32),
            pltpu.VMEM((n_tp, seqs, 8, rows), f32),
            pltpu.VMEM((seqs * rows, 128), f32),
            pltpu.VMEM((n_ctx, *w_out.shape), bf16),
            pltpu.VMEM((seqs * n_ctx, 2 * rows, HEAD_DIM), bf16),
            pltpu.VMEM((seqs * heads, rows, HEAD_DIM), bf16),
            pltpu.VMEM((heads, rows, 128), f32),
            pltpu.VMEM((heads, rows, 2 * HEAD_DIM), f32),
            pltpu.VMEM((seqs, rows, qw), bf16),
            pltpu.VMEM((n_tp * seqs, rows, depth), bf16),
            pltpu.VMEM((seqs, rows, depth), bf16),
            pltpu.VMEM((2 * seqs, rows, depth), bf16),
            pltpu.VMEM((2 * seqs, rows, depth // 2), bf16),
            pltpu.VMEM((2 * seqs, rows, depth), bf16),
            pltpu.VMEM((seqs, rows, depth), bf16),
            pltpu.SemaphoreType.DMA((144,)),
            pltpu.SemaphoreType.DMA((144,)),
            pltpu.SemaphoreType.DMA((5,)),
        ],
        compiler_params=pltpu.CompilerParams(
            collective_id=0, has_side_effects=True, vmem_limit_bytes=63 * 2**20
        ),
    )(tokens, w_query, w_key, value_weight, w_out, norm_gain.reshape(n_tp, 1, depth), cosine, sine, query_pos, key_pos)


def solution(mesh):
    placed = (
        P(None, "ctx", "tp"),
        P(),
        P(),
        P("ctx", "tp"),
        P("ctx", "tp"),
        P("ctx", "tp"),
        P("tp", "ctx"),
    )
    return jax.shard_map(
        per_device, mesh=mesh, in_specs=placed, out_specs=P(None, "ctx", "tp"), check_vma=False
    )
```

```python
import math

import jax
import jax.numpy as jnp
from jax import lax
from jax.experimental import pallas as pl
from jax.experimental.pallas import tpu as pltpu
from jax.sharding import PartitionSpec as P

HEAD_DIM = 128


theta_base = 500000.0
norm_eps = 1e-05
masked_score = -1e30


def in_one_piece(arrays, axis, dim, along):
    ends, at = ([], 0)
    for a in arrays[:-1]:
        at += a.shape[along]
        ends.append(at)
    both = jnp.concatenate(arrays, axis=along)
    return tuple(jnp.split(lax.all_gather(both, axis, axis=dim, tiled=True), ends, axis=along))


MESH = pl.DeviceIdType.MESH


def neighbours():
    ctx, tp = lax.axis_index("ctx"), lax.axis_index("tp")
    z, xl, core = ctx // 4, (ctx // 2) % 2, ctx % 2
    xh, y = tp // 4, tp % 4

    def at(z_, xl_, core_, xh_, y_):
        return {"ctx": z_ * 4 + xl_ * 2 + core_, "tp": xh_ * 4 + y_}

    return {
        "yp": at(z, xl, core, xh, (y + 1) % 4),
        "ym": at(z, xl, core, xh, (y + 3) % 4),
        "y2": at(z, xl, core, xh, (y + 2) % 4),
        "xh": at(z, xl, core, 1 - xh, y),
        "xhyp": at(z, xl, core, 1 - xh, (y + 1) % 4),
        "xhym": at(z, xl, core, 1 - xh, (y + 3) % 4),
        "xhy2": at(z, xl, core, 1 - xh, (y + 2) % 4),
        "zp": at((z + 1) % 4, xl, core, xh, y),
        "zm": at((z + 3) % 4, xl, core, xh, y),
        "xl": at(z, 1 - xl, core, xh, y),
        "co": at(z, xl, 1 - core, xh, y),
    }


class Links:
    def __init__(self, send, recv):
        self.send, self.recv, self.count = send, recv, 0
        self.where = neighbours()
        self.sent = []

    def greet(self, names):
        barrier = pltpu.get_barrier_semaphore()
        for name in names:
            pl.semaphore_signal(barrier, 1, device_id=self.where[name], device_id_type=MESH)
        pl.semaphore_wait(barrier, len(names))

    def ticket(self):
        self.count += 1
        return self.count - 1

    def copy(self, ticket, src, dst, name):
        return pltpu.make_async_remote_copy(
            src, dst, self.send.at[ticket], self.recv.at[ticket],
            device_id=self.where[name], device_id_type=MESH,
        )

    def start(self, ticket, src, dst, name):
        c = self.copy(ticket, src, dst, name)
        c.start()
        self.sent.append(c)

    def arrive(self, ticket, here, name="co"):
        self.copy(ticket, here, here, name).wait_recv()

    def finish(self):
        for c in self.sent:
            c.wait_send()
        self.sent = []


def token_flow(links, tokens_buf, source):
    tp = lax.axis_index("tp")
    xh, y = tp // 4, tp % 4

    def shard(dx, dy):
        return (xh if dx == 0 else 1 - xh) * 4 + (y + dy) % 4

    def slot(dx, dy, s, rows=None):
        ref = tokens_buf.at[shard(dx, dy) * 2 + s]
        return ref if rows is None else ref.at[pl.ds(rows[0], rows[1])]

    rows = tokens_buf.shape[1]
    low, high = (0, rows // 2), (rows // 2, rows // 2)
    T = {}
    for s in range(2):
        for k in ("yp", "ym", "xh", "fa", "fb", "pyp", "pym", "x2"):
            T[k, s] = links.ticket()
    T["pfa"], T["pfb"] = links.ticket(), links.ticket()

    def own(s, first):
        if not first:
            links.start(T["xh", s], source.at[s], slot(0, 0, s), "xh")
            return
        links.start(T["yp", s], source.at[s], slot(0, 0, s), "yp")
        links.start(T["ym", s], source.at[s], slot(0, 0, s), "ym")

    def forward(s):
        links.arrive(T["yp", s], slot(0, 3, s), "ym")
        links.start(T["fa", s], slot(0, 3, s, low), slot(0, 3, s, low), "yp")
        links.arrive(T["ym", s], slot(0, 1, s), "yp")
        links.start(T["fb", s], slot(0, 1, s, high), slot(0, 1, s, high), "ym")

    def partner(s):
        links.arrive(T["xh", s], slot(1, 0, s), "xh")
        links.start(T["pyp", s], slot(1, 0, s), slot(1, 0, s), "yp")
        links.start(T["pym", s], slot(1, 0, s), slot(1, 0, s), "ym")

    def across(s):
        links.arrive(T["fa", s], slot(0, 2, s, low), "ym")
        links.arrive(T["fb", s], slot(0, 2, s, high), "yp")
        if s == 0:
            links.start(T["x2", s], slot(0, 2, s), slot(0, 2, s), "xh")

    def sides(s):
        links.arrive(T["pyp", s], slot(1, 3, s), "ym")
        if s == 1:
            links.start(T["pfa"], slot(1, 3, s, low), slot(1, 3, s, low), "yp")
        links.arrive(T["pym", s], slot(1, 1, s), "yp")
        if s == 1:
            links.start(T["pfb"], slot(1, 1, s, high), slot(1, 1, s, high), "ym")

    def last(s):
        if s == 0:
            links.arrive(T["x2", s], slot(1, 2, s), "xh")
        else:
            links.arrive(T["pfa"], slot(1, 2, s, low), "ym")
            links.arrive(T["pfb"], slot(1, 2, s, high), "yp")

    return dict(own=own, forward=forward, partner=partner, across=across, sides=sides, last=last, shard=shard)


def squares_flow(links, buf):
    tp = lax.axis_index("tp")
    xh, y = tp // 4, tp % 4

    def slot(dx, dy):
        return buf.at[(xh if dx == 0 else 1 - xh) * 4 + (y + dy) % 4]

    routes = {"yp": (0, 3), "ym": (0, 1), "y2": (0, 2), "xh": (1, 0), "xhyp": (1, 3), "xhym": (1, 1), "xhy2": (1, 2)}
    T = {k: links.ticket() for k in routes}

    def own():
        for k in routes:
            links.start(T[k], slot(0, 0), slot(0, 0), k)

    def arrived():
        for k, where in routes.items():
            links.arrive(T[k], slot(*where))

    return {"own": own, "all": arrived}


def by_rank(z, xl, core):
    return z * 4 + xl * 2 + core


def by_pair(z, xl, core):
    return xl * 8 + z * 2 + core


def column_flow(links, buf, place=by_rank, far_by_x=False):
    ctx = lax.axis_index("ctx")
    z, xl, core = ctx // 4, (ctx // 2) % 2, ctx % 2
    rows = buf.shape[1]
    half = rows // 2

    def slot(dx, dz, dc=0, part=None):
        i = place((z + dz) % 4, xl if dx == 0 else 1 - xl, core if dc == 0 else 1 - core)
        ref = buf.at[i]
        return ref if part is None else ref.at[pl.ds(part * half, half)]

    T = {}
    for k in ("zp", "zm", "xl0", "xl1", "fa", "fb", "pzp0", "pzp1", "pzm0", "pzm1", "pfa", "pfb", "x2"):
        T[k] = links.ticket()
    for dx in range(2):
        for dz in range(4):
            T["co", dx, dz] = links.ticket()

    def share(dx, dz):
        links.start(T["co", dx, dz], slot(dx, dz), slot(dx, dz), "co")

    def own_x(part):
        links.start(T[f"xl{part}"], slot(0, 0, 0, part), slot(0, 0, 0, part), "xl")

    def own_z():
        links.start(T["zp"], slot(0, 0), slot(0, 0), "zp")
        links.start(T["zm"], slot(0, 0), slot(0, 0), "zm")
        share(0, 0)

    def forward():
        links.arrive(T["zp"], slot(0, 3), "zm")
        links.start(T["fa"], slot(0, 3, 0, 0), slot(0, 3, 0, 0), "zp")
        links.arrive(T["zm"], slot(0, 1), "zp")
        links.start(T["fb"], slot(0, 1, 0, 1), slot(0, 1, 0, 1), "zm")
        share(0, 3)
        share(0, 1)

    def partner(part):
        links.arrive(T[f"xl{part}"], slot(1, 0, 0, part), "xl")
        links.start(T[f"pzp{part}"], slot(1, 0, 0, part), slot(1, 0, 0, part), "zp")
        links.start(T[f"pzm{part}"], slot(1, 0, 0, part), slot(1, 0, 0, part), "zm")
        if part == 1:
            share(1, 0)

    def across():
        links.arrive(T["fa"], slot(0, 2, 0, 0), "zm")
        links.arrive(T["fb"], slot(0, 2, 0, 1), "zp")
        if far_by_x:
            links.start(T["x2"], slot(0, 2), slot(0, 2), "xl")
        share(0, 2)

    def sides():
        if far_by_x:
            for part in range(2):
                links.arrive(T[f"pzp{part}"], slot(1, 3, 0, part), "zm")
                links.arrive(T[f"pzm{part}"], slot(1, 1, 0, part), "zp")
            share(1, 3)
            share(1, 1)
            return
        links.arrive(T["pzp0"], slot(1, 3, 0, 0), "zm")
        links.start(T["pfa"], slot(1, 3, 0, 0), slot(1, 3, 0, 0), "zp")
        links.arrive(T["pzm0"], slot(1, 1, 0, 0), "zp")
        links.arrive(T["pzm1"], slot(1, 1, 0, 1), "zp")
        links.start(T["pfb"], slot(1, 1, 0, 1), slot(1, 1, 0, 1), "zm")
        links.arrive(T["pzp1"], slot(1, 3, 0, 1), "zm")
        share(1, 3)
        share(1, 1)

    def last():
        if far_by_x:
            links.arrive(T["x2"], slot(1, 2), "xl")
            share(1, 2)
            return
        links.arrive(T["pfa"], slot(1, 2, 0, 0), "zm")
        links.arrive(T["pfb"], slot(1, 2, 0, 1), "zp")
        share(1, 2)

    def shared(pairs):
        for dx, dz in pairs:
            links.arrive(T["co", dx, dz], slot(dx, dz, 1), "co")

    everything = [(dx, dz) for dx in range(2) for dz in range(4)]
    return dict(own_x=own_x, own_z=own_z, forward=forward, partner=partner, across=across, sides=sides,
                last=last, shared=shared, everything=everything)


def attend(s, first_pair, pair, q_buf, kv_buf, query_pos, key_pos, peaks, sums, out):
    rows = q_buf.shape[1]
    heads = out.shape[2] // HEAD_DIM
    scale = math.log2(math.e) / math.sqrt(HEAD_DIM)

    def body(h, _):
        i = s * heads + h
        held = pl.ds(s * 16 + pair * 8, 8)
        keys = kv_buf[held, :rows, :].reshape(8 * rows, HEAD_DIM)
        values = kv_buf[held, rows:, :].reshape(8 * rows, HEAD_DIM)
        scores = lax.dot_general(
            q_buf[i], keys, (((1,), (1,)), ((), ())), preferred_element_type=jnp.float32
        )
        allowed = key_pos[s * 2 + pair] <= query_pos[s, :, :1]
        scores = jnp.where(allowed, scores, masked_score)
        peak = jnp.maximum(jnp.max(scores, axis=1, keepdims=True), 1e-10 * masked_score)
        if not first_pair:
            before = peaks[h, :, :1]
            peak = jnp.maximum(peak, before)
        weights = jnp.exp2((scores - peak) * scale).astype(jnp.bfloat16)
        both = jnp.concatenate([values, jnp.ones_like(values)], axis=1)
        summed = jnp.dot(weights, both, preferred_element_type=jnp.float32)
        if first_pair:
            peaks[h] = jnp.broadcast_to(peak, peaks.shape[1:])
            sums[h] = summed
        else:
            summed = summed + sums[h] * jnp.exp2((before - peak) * scale)
            mean = summed[:, :HEAD_DIM] / summed[:, HEAD_DIM:]
            out[s, :, pl.ds(pl.multiple_of(h * HEAD_DIM, HEAD_DIM), HEAD_DIM)] = mean.astype(jnp.bfloat16)
        return 0

    lax.fori_loop(0, heads, body, 0)


def mix_kernel(tokens, wq, wk, wv, wo, span_order, gain, freqs, mixed,
               cosine, sine, query_pos, key_pos, tbuf, wbuf, acc, squares, factors, wobuf, kvbuf, qbuf, peaks, sums, attended,
               terms, from_x, from_y, halves, last_y, last_x, send, recv, local):
    links = Links(send, recv)
    ctx, tp = lax.axis_index("ctx"), lax.axis_index("tp")
    z, xl, core = ctx // 4, (ctx // 2) % 2, ctx % 2
    rows = tokens.shape[1]
    qw, kw = wq.shape[1], wk.shape[1]
    width = qw + 2 * kw
    heads = qw // HEAD_DIM
    mine = [
        pltpu.make_async_copy(tokens, tbuf.at[pl.ds(tp * 2, 2)], local.at[3]),
        pltpu.make_async_copy(wq, wbuf.at[ctx, :, pl.ds(0, qw)], local.at[0]),
        pltpu.make_async_copy(wk, wbuf.at[ctx, :, pl.ds(qw, kw)], local.at[1]),
        pltpu.make_async_copy(wv, wbuf.at[ctx, :, pl.ds(qw + kw, kw)], local.at[2]),
        pltpu.make_async_copy(wo, wobuf.at[ctx], local.at[4]),
    ]
    for c in mine:
        c.start()
    t = token_flow(links, tbuf, tokens)
    w = column_flow(links, wbuf)
    statistics = squares_flow(links, squares)
    o = column_flow(links, wobuf, far_by_x=True)
    kv = [
        column_flow(links, kvbuf, lambda z_, xl_, core_, s=s: s * 16 + by_pair(z_, xl_, core_), far_by_x=True)
        for s in range(2)
    ]
    links.greet(("yp", "ym", "y2", "xh", "xhyp", "xhym", "xhy2", "zp", "zm", "xl", "co"))
    t["own"](0, first=True)
    for c in mine[1:4]:
        c.wait()
    w["own_x"](0)
    w["own_z"]()
    t["own"](1, first=False)
    w["own_x"](1)
    t["own"](1, first=True)
    t["own"](0, first=False)
    mine[0].wait()
    for s in range(2):
        wide = tbuf[tp * 2 + s].astype(jnp.float32)
        squares[tp, s] = lax.dot_general(
            jnp.ones((8, wide.shape[1]), jnp.float32), wide * wide, (((1,), (1,)), ((), ())),
            precision=lax.Precision.HIGHEST, preferred_element_type=jnp.float32,
        )
    statistics["own"]()
    acc[...] = jnp.zeros_like(acc)
    mine[4].wait()

    def multiply(shard):
        wide = tbuf[pl.ds(shard * 2, 2)].astype(jnp.float32).reshape(2 * rows, tokens.shape[2])
        x = (wide * factors[:, :1] * gain[shard]).astype(jnp.bfloat16)
        weights = wbuf[pl.ds(2 * shard, 2)].reshape(x.shape[1], width)
        acc[...] += jnp.dot(x, weights, preferred_element_type=jnp.float32)

    def run(dx, first, count, stride=1):
        def body(i, _):
            multiply((tp // 4 + dx) % 2 * 4 + (tp % 4 + first + stride * i) % 4)
            return 0

        lax.fori_loop(0, count, body, 0)

    block_rows = 16 * rows // span_order.shape[1]
    per_rank = rows // block_rows
    lane = lax.broadcasted_iota(jnp.int32, (1, block_rows), 1)
    down = lax.broadcasted_iota(jnp.int32, (block_rows, HEAD_DIM), 0)
    sign = jnp.where(lax.broadcasted_iota(jnp.int32, (1, HEAD_DIM), 1) < HEAD_DIM // 2, -1.0, 1.0)
    for s in range(2):
        for i in range(16 * per_rank):
            rank, part = i // per_rank, i % per_rank
            at = ((rank // 4 * 2 + rank % 2) * per_rank + part) * block_rows
            key_pos[s * 2 + rank // 2 % 2, :, at:at + block_rows] = span_order[s, i] * block_rows + lane
        for part in range(per_rank):
            at = slice(part * block_rows, (part + 1) * block_rows)
            position = span_order[s, ctx * per_rank + part] * block_rows + down
            query_pos[s, at] = position
            angle = position.astype(jnp.float32) * freqs[...]
            cosine[s, at] = jnp.cos(angle)
            sine[s, at] = jnp.sin(angle) * sign

    own_column, other_column = [[(dx, dz) for dz in range(4)] for dx in range(2)]
    near = (xl + tp % 4) % 2
    t["forward"](0)
    w["partner"](0)
    w["forward"]()
    t["forward"](1)
    t["partner"](1)
    w["across"]()
    w["partner"](1)
    t["across"](0)
    t["across"](1)
    o["own_x"](0)
    o["own_x"](1)
    statistics["all"]()
    features = 8 * tokens.shape[2]
    for s in range(2):
        total = squares[0, s]
        for i in range(1, 8):
            total = total + squares[i, s]
        factor = lax.rsqrt(total[:1] * (1.0 / features) + norm_eps)
        factors[s * rows:(s + 1) * rows] = jnp.transpose(jnp.broadcast_to(factor, (128, rows)))
    w["shared"](own_column)
    t["partner"](0)
    run(0, near, 2, 2)
    w["sides"]()
    o["own_z"]()
    t["sides"](1)
    w["last"]()
    w["shared"](other_column)
    run(0, 1 - near, 2, 2)
    run(1, 0, 1)
    t["sides"](0)
    run(1, 1, 2, 2)
    t["last"](0)
    t["last"](1)
    o["forward"]()
    run(1, 2, 1)

    own = by_pair(z, xl, core)

    def turn(x, s):
        return x * cosine[s] + pltpu.roll(x, HEAD_DIM // 2, 1) * sine[s]

    for s in range(2):
        at = pl.ds(s * rows, rows)
        kvbuf[s * 16 + own, :rows] = turn(acc[at, qw:qw + kw], s).astype(jnp.bfloat16)
        kvbuf[s * 16 + own, rows:] = acc[at, qw + kw:].astype(jnp.bfloat16)
    for s in range(2):
        kv[s]["own_x"](0)
        kv[s]["own_z"]()
        kv[s]["own_x"](1)
    for s in range(2):
        for h in range(heads):
            qbuf[s * heads + h] = turn(acc[pl.ds(s * rows, rows), h * HEAD_DIM:(h + 1) * HEAD_DIM], s).astype(jnp.bfloat16)

    def look(s, first_pair):
        attend(s, first_pair, xl if first_pair else 1 - xl, qbuf, kvbuf, query_pos, key_pos, peaks, sums, attended)

    half = mixed.shape[2] // 2
    cut = [pl.ds(0, half), pl.ds(half, half)]

    def term(dx, dy, s):
        return (dx * 4 + dy) * 2 + s

    def products(s, first, count):
        def body(i, _):
            rel = first + i
            block = (tp // 4 + rel // 4) % 2 * 4 + (tp % 4 + rel % 4) % 4
            for c in range(2):
                terms[rel * 2 + s, :, c * half:(c + 1) * half] = jnp.dot(
                    attended[s], wobuf[2 * block + c], preferred_element_type=jnp.float32
                ).astype(jnp.bfloat16)
            return 0

        lax.fori_loop(0, count, body, 0)

    R = {(k, s): links.ticket() for s in range(2) for k in ("x", "yp", "ym", "h0", "h1", "zyp0", "zyp1", "zym0", "zym1", "zx")}

    def wide(ref):
        return ref[...].astype(jnp.float32)

    def open_sums(s):
        products(s, 6, 1)
        links.start(R["x", s], terms.at[term(1, 2, s)], from_x.at[s], "xh")
        products(s, 5, 1)
        links.start(R["yp", s], terms.at[term(1, 1, s)], from_y.at[s], "yp")
        products(s, 7, 1)
        links.start(R["ym", s], terms.at[term(1, 3, s)], from_y.at[2 + s], "ym")
        products(s, 0, 5)

    def far(s):
        links.arrive(R["x", s], from_x.at[s])
        here = terms.at[term(0, 2, s)]
        here[...] = (wide(here) + wide(from_x.at[s])).astype(jnp.bfloat16)
        for c, to in ((0, "yp"), (1, "ym")):
            links.start(R[f"h{c}", s], here.at[:, cut[c]], halves.at[2 * c + s], to)
        links.start(R["zyp1", s], terms.at[term(0, 1, s), :, cut[1]], last_y.at[s, :, cut[1]], "yp")
        links.start(R["zym0", s], terms.at[term(0, 3, s), :, cut[0]], last_y.at[2 + s, :, cut[0]], "ym")

    def over(s):
        links.arrive(R["yp", s], from_y.at[s])
        links.arrive(R["ym", s], from_y.at[2 + s])
        here = terms.at[term(1, 0, s)]
        here[...] = (wide(here) + wide(from_y.at[s]) + wide(from_y.at[2 + s])).astype(jnp.bfloat16)
        links.start(R["zx", s], here, last_x.at[s], "xh")

    def close(s):
        for c, dy, k, to in ((0, 1, "zyp0", "yp"), (1, 3, "zym1", "ym")):
            links.arrive(R[f"h{c}", s], halves.at[2 * c + s])
            here = terms.at[term(0, dy, s), :, cut[c]]
            here[...] = (wide(here) + wide(halves.at[2 * c + s])).astype(jnp.bfloat16)
            links.start(R[k, s], here, last_y.at[2 * c + s, :, cut[c]], to)

    def result(s):
        links.arrive(R["zx", s], last_x.at[s])
        for c in range(2):
            links.arrive(R[f"zyp{c}", s], last_y.at[s, :, cut[c]])
            links.arrive(R[f"zym{c}", s], last_y.at[2 + s, :, cut[c]])
        total = wide(terms.at[term(0, 0, s)]) + wide(last_x.at[s]) + wide(last_y.at[s]) + wide(last_y.at[2 + s])
        mixed[s] = total.astype(jnp.bfloat16)

    for s in range(2):
        kv[s]["partner"](0)
        kv[s]["forward"]()
        kv[s]["partner"](1)
    o["partner"](0)
    o["partner"](1)
    for s in range(2):
        kv[s]["across"]()
    o["across"]()
    kv[0]["shared"](own_column)
    look(0, True)
    kv[0]["sides"]()
    kv[1]["sides"]()
    kv[0]["last"]()
    kv[1]["last"]()
    kv[0]["shared"](other_column)
    look(0, False)
    o["sides"]()
    o["last"]()
    o["shared"](own_column + other_column)
    open_sums(0)
    kv[1]["shared"](own_column)
    look(1, True)
    far(0)
    over(0)
    kv[1]["shared"](other_column)
    look(1, False)
    open_sums(1)
    close(0)
    far(1)
    over(1)
    close(1)
    result(0)
    result(1)
    links.finish()


def per_device(tokens, norm_gain, span_order, w_query, w_key, value_weight, w_out):
    n_ctx, n_tp = 16, 8
    seqs, rows, depth = tokens.shape
    qw = w_query.shape[1]
    width = qw + w_key.shape[1] + value_weight.shape[1]
    heads = qw // HEAD_DIM
    bf16, f32, i32 = jnp.bfloat16, jnp.float32, jnp.int32
    order = jnp.arange(HEAD_DIM // 2, dtype=f32)
    freqs = jnp.exp(-(2.0 * order / HEAD_DIM) * math.log(theta_base))
    freqs = jnp.concatenate([freqs, freqs])[None]
    anyspace = pl.BlockSpec(memory_space=pl.ANY)
    vmem = pl.BlockSpec(memory_space=pltpu.VMEM)
    return pl.pallas_call(
        mix_kernel,
        out_shape=jax.ShapeDtypeStruct(tokens.shape, bf16),
        in_specs=[anyspace] * 5 + [pl.BlockSpec(memory_space=pltpu.SMEM)] + [vmem] * 2,
        out_specs=vmem,
        scratch_shapes=[
            pltpu.VMEM((seqs, rows, HEAD_DIM), f32),
            pltpu.VMEM((seqs, rows, HEAD_DIM), f32),
            pltpu.VMEM((seqs, rows, 128), i32),
            pltpu.VMEM((2 * seqs, 1, 8 * rows), i32),
            pltpu.VMEM((n_tp * seqs, rows, depth), bf16),
            pltpu.VMEM((n_ctx, w_query.shape[0], width), bf16),
            pltpu.VMEM((seqs * rows, width), f32),
            pltpu.VMEM((n_tp, seqs, 8, rows), f32),
            pltpu.VMEM((seqs * rows, 128), f32),
            pltpu.VMEM((n_ctx, *w_out.shape), bf16),
            pltpu.VMEM((seqs * n_ctx, 2 * rows, HEAD_DIM), bf16),
            pltpu.VMEM((seqs * heads, rows, HEAD_DIM), bf16),
            pltpu.VMEM((heads, rows, 128), f32),
            pltpu.VMEM((heads, rows, 2 * HEAD_DIM), f32),
            pltpu.VMEM((seqs, rows, qw), bf16),
            pltpu.VMEM((n_tp * seqs, rows, depth), bf16),
            pltpu.VMEM((seqs, rows, depth), bf16),
            pltpu.VMEM((2 * seqs, rows, depth), bf16),
            pltpu.VMEM((2 * seqs, rows, depth // 2), bf16),
            pltpu.VMEM((2 * seqs, rows, depth), bf16),
            pltpu.VMEM((seqs, rows, depth), bf16),
            pltpu.SemaphoreType.DMA((144,)),
            pltpu.SemaphoreType.DMA((144,)),
            pltpu.SemaphoreType.DMA((5,)),
        ],
        compiler_params=pltpu.CompilerParams(
            collective_id=0, has_side_effects=True, vmem_limit_bytes=63 * 2**20
        ),
    )(tokens, w_query, w_key, value_weight, w_out, span_order, norm_gain.reshape(n_tp, 1, depth), freqs)


def solution(mesh):
    placed = (
        P(None, "ctx", "tp"),
        P(),
        P(),
        P("ctx", "tp"),
        P("ctx", "tp"),
        P("ctx", "tp"),
        P("tp", "ctx"),
    )
    return jax.shard_map(
        per_device, mesh=mesh, in_specs=placed, out_specs=P(None, "ctx", "tp"), check_vma=False
    )
```

```python
import math

import jax
import jax.numpy as jnp
from jax import lax
from jax.experimental import pallas as pl
from jax.experimental.pallas import tpu as pltpu
from jax.sharding import PartitionSpec as P

HEAD_DIM = 128


theta_base = 500000.0
norm_eps = 1e-05
masked_score = -1e30


def in_one_piece(arrays, axis, dim, along):
    ends, at = ([], 0)
    for a in arrays[:-1]:
        at += a.shape[along]
        ends.append(at)
    both = jnp.concatenate(arrays, axis=along)
    return tuple(jnp.split(lax.all_gather(both, axis, axis=dim, tiled=True), ends, axis=along))


MESH = pl.DeviceIdType.MESH


def neighbours():
    ctx, tp = lax.axis_index("ctx"), lax.axis_index("tp")
    z, xl, core = ctx // 4, (ctx // 2) % 2, ctx % 2
    xh, y = tp // 4, tp % 4

    def at(z_, xl_, core_, xh_, y_):
        return {"ctx": z_ * 4 + xl_ * 2 + core_, "tp": xh_ * 4 + y_}

    return {
        "yp": at(z, xl, core, xh, (y + 1) % 4),
        "ym": at(z, xl, core, xh, (y + 3) % 4),
        "y2": at(z, xl, core, xh, (y + 2) % 4),
        "xh": at(z, xl, core, 1 - xh, y),
        "xhyp": at(z, xl, core, 1 - xh, (y + 1) % 4),
        "xhym": at(z, xl, core, 1 - xh, (y + 3) % 4),
        "xhy2": at(z, xl, core, 1 - xh, (y + 2) % 4),
        "zp": at((z + 1) % 4, xl, core, xh, y),
        "zm": at((z + 3) % 4, xl, core, xh, y),
        "xl": at(z, 1 - xl, core, xh, y),
        "co": at(z, xl, 1 - core, xh, y),
    }


class Links:
    def __init__(self, send, recv):
        self.send, self.recv, self.count = send, recv, 0
        self.where = neighbours()
        self.sent = []

    def greet(self, names):
        barrier = pltpu.get_barrier_semaphore()
        for name in names:
            pl.semaphore_signal(barrier, 1, device_id=self.where[name], device_id_type=MESH)
        pl.semaphore_wait(barrier, len(names))

    def ticket(self):
        self.count += 1
        return self.count - 1

    def copy(self, ticket, src, dst, name):
        return pltpu.make_async_remote_copy(
            src, dst, self.send.at[ticket], self.recv.at[ticket],
            device_id=self.where[name], device_id_type=MESH,
        )

    def start(self, ticket, src, dst, name):
        c = self.copy(ticket, src, dst, name)
        c.start()
        self.sent.append(c)

    def arrive(self, ticket, here, name="co"):
        self.copy(ticket, here, here, name).wait_recv()

    def finish(self):
        for c in self.sent:
            c.wait_send()
        self.sent = []


def token_flow(links, tokens_buf, source):
    tp = lax.axis_index("tp")
    xh, y = tp // 4, tp % 4

    def shard(dx, dy):
        return (xh if dx == 0 else 1 - xh) * 4 + (y + dy) % 4

    def slot(dx, dy, s, rows=None):
        ref = tokens_buf.at[shard(dx, dy) * 2 + s]
        return ref if rows is None else ref.at[pl.ds(rows[0], rows[1])]

    rows = tokens_buf.shape[1]
    low, high = (0, rows // 2), (rows // 2, rows // 2)
    T = {}
    for s in range(2):
        for k in ("yp", "ym", "xh", "fa", "fb", "pyp", "pym", "x2"):
            T[k, s] = links.ticket()
    T["pfa"], T["pfb"] = links.ticket(), links.ticket()

    def own(s, first):
        if not first:
            links.start(T["xh", s], source.at[s], slot(0, 0, s), "xh")
            return
        links.start(T["yp", s], source.at[s], slot(0, 0, s), "yp")
        links.start(T["ym", s], source.at[s], slot(0, 0, s), "ym")

    def forward(s):
        links.arrive(T["yp", s], slot(0, 3, s), "ym")
        links.start(T["fa", s], slot(0, 3, s, low), slot(0, 3, s, low), "yp")
        links.arrive(T["ym", s], slot(0, 1, s), "yp")
        links.start(T["fb", s], slot(0, 1, s, high), slot(0, 1, s, high), "ym")

    def partner(s):
        links.arrive(T["xh", s], slot(1, 0, s), "xh")
        links.start(T["pyp", s], slot(1, 0, s), slot(1, 0, s), "yp")
        links.start(T["pym", s], slot(1, 0, s), slot(1, 0, s), "ym")

    def across(s):
        links.arrive(T["fa", s], slot(0, 2, s, low), "ym")
        links.arrive(T["fb", s], slot(0, 2, s, high), "yp")
        if s == 0:
            links.start(T["x2", s], slot(0, 2, s), slot(0, 2, s), "xh")

    def sides(s):
        links.arrive(T["pyp", s], slot(1, 3, s), "ym")
        if s == 1:
            links.start(T["pfa"], slot(1, 3, s, low), slot(1, 3, s, low), "yp")
        links.arrive(T["pym", s], slot(1, 1, s), "yp")
        if s == 1:
            links.start(T["pfb"], slot(1, 1, s, high), slot(1, 1, s, high), "ym")

    def last(s):
        if s == 0:
            links.arrive(T["x2", s], slot(1, 2, s), "xh")
        else:
            links.arrive(T["pfa"], slot(1, 2, s, low), "ym")
            links.arrive(T["pfb"], slot(1, 2, s, high), "yp")

    return dict(own=own, forward=forward, partner=partner, across=across, sides=sides, last=last, shard=shard)


def squares_flow(links, buf):
    tp = lax.axis_index("tp")
    xh, y = tp // 4, tp % 4

    def slot(dx, dy):
        return buf.at[(xh if dx == 0 else 1 - xh) * 4 + (y + dy) % 4]

    routes = {"yp": (0, 3), "ym": (0, 1), "y2": (0, 2), "xh": (1, 0), "xhyp": (1, 3), "xhym": (1, 1), "xhy2": (1, 2)}
    T = {k: links.ticket() for k in routes}

    def own():
        for k in routes:
            links.start(T[k], slot(0, 0), slot(0, 0), k)

    def arrived():
        for k, where in routes.items():
            links.arrive(T[k], slot(*where))

    return {"own": own, "all": arrived}


def by_rank(z, xl, core):
    return z * 4 + xl * 2 + core


def by_pair(z, xl, core):
    return xl * 8 + z * 2 + core


def column_flow(links, buf, place=by_rank, far_by_x=False):
    ctx = lax.axis_index("ctx")
    z, xl, core = ctx // 4, (ctx // 2) % 2, ctx % 2
    rows = buf.shape[1]
    half = rows // 2

    def slot(dx, dz, dc=0, part=None):
        i = place((z + dz) % 4, xl if dx == 0 else 1 - xl, core if dc == 0 else 1 - core)
        ref = buf.at[i]
        return ref if part is None else ref.at[pl.ds(part * half, half)]

    T = {}
    for k in ("zp", "zm", "xl0", "xl1", "fa", "fb", "pzp0", "pzp1", "pzm0", "pzm1", "pfa", "pfb", "x2"):
        T[k] = links.ticket()
    for dx in range(2):
        for dz in range(4):
            T["co", dx, dz] = links.ticket()

    def share(dx, dz):
        links.start(T["co", dx, dz], slot(dx, dz), slot(dx, dz), "co")

    def own_x(part):
        links.start(T[f"xl{part}"], slot(0, 0, 0, part), slot(0, 0, 0, part), "xl")

    def own_z():
        links.start(T["zp"], slot(0, 0), slot(0, 0), "zp")
        links.start(T["zm"], slot(0, 0), slot(0, 0), "zm")
        share(0, 0)

    def forward():
        links.arrive(T["zp"], slot(0, 3), "zm")
        links.start(T["fa"], slot(0, 3, 0, 0), slot(0, 3, 0, 0), "zp")
        links.arrive(T["zm"], slot(0, 1), "zp")
        links.start(T["fb"], slot(0, 1, 0, 1), slot(0, 1, 0, 1), "zm")
        share(0, 3)
        share(0, 1)

    def partner(part):
        links.arrive(T[f"xl{part}"], slot(1, 0, 0, part), "xl")
        links.start(T[f"pzp{part}"], slot(1, 0, 0, part), slot(1, 0, 0, part), "zp")
        links.start(T[f"pzm{part}"], slot(1, 0, 0, part), slot(1, 0, 0, part), "zm")
        if part == 1:
            share(1, 0)

    def across():
        links.arrive(T["fa"], slot(0, 2, 0, 0), "zm")
        links.arrive(T["fb"], slot(0, 2, 0, 1), "zp")
        if far_by_x:
            links.start(T["x2"], slot(0, 2), slot(0, 2), "xl")
        share(0, 2)

    def sides():
        if far_by_x:
            for part in range(2):
                links.arrive(T[f"pzp{part}"], slot(1, 3, 0, part), "zm")
                links.arrive(T[f"pzm{part}"], slot(1, 1, 0, part), "zp")
            share(1, 3)
            share(1, 1)
            return
        links.arrive(T["pzp0"], slot(1, 3, 0, 0), "zm")
        links.start(T["pfa"], slot(1, 3, 0, 0), slot(1, 3, 0, 0), "zp")
        links.arrive(T["pzm0"], slot(1, 1, 0, 0), "zp")
        links.arrive(T["pzm1"], slot(1, 1, 0, 1), "zp")
        links.start(T["pfb"], slot(1, 1, 0, 1), slot(1, 1, 0, 1), "zm")
        links.arrive(T["pzp1"], slot(1, 3, 0, 1), "zm")
        share(1, 3)
        share(1, 1)

    def last():
        if far_by_x:
            links.arrive(T["x2"], slot(1, 2), "xl")
            share(1, 2)
            return
        links.arrive(T["pfa"], slot(1, 2, 0, 0), "zm")
        links.arrive(T["pfb"], slot(1, 2, 0, 1), "zp")
        share(1, 2)

    def shared(pairs):
        for dx, dz in pairs:
            links.arrive(T["co", dx, dz], slot(dx, dz, 1), "co")

    everything = [(dx, dz) for dx in range(2) for dz in range(4)]
    return dict(own_x=own_x, own_z=own_z, forward=forward, partner=partner, across=across, sides=sides,
                last=last, shared=shared, everything=everything)


def attend(s, first_pair, pair, q_buf, kv_buf, query_pos, key_pos, peaks, sums, out):
    rows = q_buf.shape[1]
    heads = out.shape[2] // HEAD_DIM
    scale = math.log2(math.e) / math.sqrt(HEAD_DIM)

    def body(h, _):
        i = s * heads + h
        held = pl.ds(s * 16 + pair * 8, 8)
        keys = kv_buf[held, :rows, :].reshape(8 * rows, HEAD_DIM)
        values = kv_buf[held, rows:, :].reshape(8 * rows, HEAD_DIM)
        scores = lax.dot_general(
            q_buf[i], keys, (((1,), (1,)), ((), ())), preferred_element_type=jnp.float32
        )
        allowed = key_pos[s * 2 + pair] <= query_pos[s, :, :1]
        scores = jnp.where(allowed, scores, masked_score)
        peak = jnp.maximum(jnp.max(scores, axis=1, keepdims=True), 1e-10 * masked_score)
        if not first_pair:
            before = peaks[h, :, :1]
            peak = jnp.maximum(peak, before)
        weights = jnp.exp2((scores - peak) * scale).astype(jnp.bfloat16)
        both = jnp.concatenate([values, jnp.ones_like(values)], axis=1)
        summed = jnp.dot(weights, both, preferred_element_type=jnp.float32)
        if first_pair:
            peaks[h] = jnp.broadcast_to(peak, peaks.shape[1:])
            sums[h] = summed
        else:
            summed = summed + sums[h] * jnp.exp2((before - peak) * scale)
            mean = summed[:, :HEAD_DIM] / summed[:, HEAD_DIM:]
            out[s, :, pl.ds(pl.multiple_of(h * HEAD_DIM, HEAD_DIM), HEAD_DIM)] = mean.astype(jnp.bfloat16)
        return 0

    lax.fori_loop(0, heads, body, 0)


def mix_kernel(tokens, wq, wk, wv, wo, span_order, gain, freqs, mixed,
               cosine, sine, query_pos, key_pos, tbuf, wbuf, acc, squares, factors, wobuf, kvbuf, qbuf, peaks, sums, attended,
               terms, from_x, from_y, halves, last_y, last_x, send, recv, local):
    links = Links(send, recv)
    ctx, tp = lax.axis_index("ctx"), lax.axis_index("tp")
    z, xl, core = ctx // 4, (ctx // 2) % 2, ctx % 2
    rows = tokens.shape[1]
    qw, kw = wq.shape[1], wk.shape[1]
    width = qw + 2 * kw
    heads = qw // HEAD_DIM
    mine = [
        pltpu.make_async_copy(tokens, tbuf.at[pl.ds(tp * 2, 2)], local.at[3]),
        pltpu.make_async_copy(wq, wbuf.at[ctx, :, pl.ds(0, qw)], local.at[0]),
        pltpu.make_async_copy(wk, wbuf.at[ctx, :, pl.ds(qw, kw)], local.at[1]),
        pltpu.make_async_copy(wv, wbuf.at[ctx, :, pl.ds(qw + kw, kw)], local.at[2]),
        pltpu.make_async_copy(wo, wobuf.at[ctx], local.at[4]),
    ]
    for c in mine:
        c.start()
    t = token_flow(links, tbuf, tokens)
    w = column_flow(links, wbuf)
    statistics = squares_flow(links, squares)
    o = column_flow(links, wobuf, far_by_x=True)
    kv = [
        column_flow(links, kvbuf, lambda z_, xl_, core_, s=s: s * 16 + by_pair(z_, xl_, core_), far_by_x=True)
        for s in range(2)
    ]
    links.greet(("yp", "ym", "y2", "xh", "xhyp", "xhym", "xhy2", "zp", "zm", "xl", "co"))
    t["own"](0, first=True)
    for c in mine[1:4]:
        c.wait()
    w["own_x"](0)
    w["own_z"]()
    t["own"](1, first=False)
    w["own_x"](1)
    t["own"](1, first=True)
    t["own"](0, first=False)
    mine[0].wait()
    for s in range(2):
        wide = tbuf[tp * 2 + s].astype(jnp.float32)
        squares[tp, s] = lax.dot_general(
            jnp.ones((8, wide.shape[1]), jnp.float32), wide * wide, (((1,), (1,)), ((), ())),
            precision=lax.Precision.HIGHEST, preferred_element_type=jnp.float32,
        )
    statistics["own"]()
    acc[...] = jnp.zeros_like(acc)
    mine[4].wait()

    def multiply(shard):
        wide = tbuf[pl.ds(shard * 2, 2)].astype(jnp.float32).reshape(2 * rows, tokens.shape[2])
        x = (wide * factors[:, :1] * gain[shard]).astype(jnp.bfloat16)
        weights = wbuf[pl.ds(2 * shard, 2)].reshape(x.shape[1], width)
        acc[...] += jnp.dot(x, weights, preferred_element_type=jnp.float32)

    def run(dx, first, count, stride=1):
        def body(i, _):
            multiply((tp // 4 + dx) % 2 * 4 + (tp % 4 + first + stride * i) % 4)
            return 0

        lax.fori_loop(0, count, body, 0)

    block_rows = 16 * rows // span_order.shape[1]
    per_rank = rows // block_rows
    lane = lax.broadcasted_iota(jnp.int32, (1, block_rows), 1)
    down = lax.broadcasted_iota(jnp.int32, (block_rows, HEAD_DIM), 0)
    sign = jnp.where(lax.broadcasted_iota(jnp.int32, (1, HEAD_DIM), 1) < HEAD_DIM // 2, -1.0, 1.0)
    for s in range(2):
        for i in range(16 * per_rank):
            rank, part = i // per_rank, i % per_rank
            at = ((rank // 4 * 2 + rank % 2) * per_rank + part) * block_rows
            key_pos[s * 2 + rank // 2 % 2, :, at:at + block_rows] = span_order[s, i] * block_rows + lane
        for part in range(per_rank):
            at = slice(part * block_rows, (part + 1) * block_rows)
            position = span_order[s, ctx * per_rank + part] * block_rows + down
            query_pos[s, at] = position
            angle = position.astype(jnp.float32) * freqs[...]
            cosine[s, at] = jnp.cos(angle)
            sine[s, at] = jnp.sin(angle) * sign

    own_column, other_column = [[(dx, dz) for dz in range(4)] for dx in range(2)]
    near = (xl + tp % 4) % 2
    t["forward"](0)
    w["partner"](0)
    w["forward"]()
    t["forward"](1)
    t["partner"](1)
    w["across"]()
    w["partner"](1)
    t["across"](0)
    t["across"](1)
    o["own_x"](0)
    o["own_x"](1)
    statistics["all"]()
    features = 8 * tokens.shape[2]
    for s in range(2):
        total = squares[0, s]
        for i in range(1, 8):
            total = total + squares[i, s]
        factor = lax.rsqrt(total[:1] * (1.0 / features) + norm_eps)
        factors[s * rows:(s + 1) * rows] = jnp.transpose(jnp.broadcast_to(factor, (128, rows)))
    w["shared"](own_column)
    t["partner"](0)
    run(0, near, 2, 2)
    w["sides"]()
    o["own_z"]()
    t["sides"](1)
    w["last"]()
    w["shared"](other_column)
    run(0, 1 - near, 2, 2)
    run(1, 0, 1)
    t["sides"](0)
    run(1, 1, 2, 2)
    t["last"](0)
    t["last"](1)
    o["forward"]()
    run(1, 2, 1)

    own = by_pair(z, xl, core)

    def turn(x, s):
        return x * cosine[s] + pltpu.roll(x, HEAD_DIM // 2, 1) * sine[s]

    for s in range(2):
        at = pl.ds(s * rows, rows)
        kvbuf[s * 16 + own, :rows] = turn(acc[at, qw:qw + kw], s).astype(jnp.bfloat16)
        kvbuf[s * 16 + own, rows:] = acc[at, qw + kw:].astype(jnp.bfloat16)
    for s in range(2):
        kv[s]["own_x"](0)
        kv[s]["own_z"]()
        kv[s]["own_x"](1)
    for s in range(2):
        for h in range(heads):
            qbuf[s * heads + h] = turn(acc[pl.ds(s * rows, rows), h * HEAD_DIM:(h + 1) * HEAD_DIM], s).astype(jnp.bfloat16)

    def look(s, first_pair):
        attend(s, first_pair, xl if first_pair else 1 - xl, qbuf, kvbuf, query_pos, key_pos, peaks, sums, attended)

    half = mixed.shape[2] // 2
    cut = [pl.ds(0, half), pl.ds(half, half)]

    def term(dx, dy, s):
        return (dx * 4 + dy) * 2 + s

    def products(s, first, count):
        def body(i, _):
            rel = first + i
            block = (tp // 4 + rel // 4) % 2 * 4 + (tp % 4 + rel % 4) % 4
            for c in range(2):
                terms[rel * 2 + s, :, c * half:(c + 1) * half] = jnp.dot(
                    attended[s], wobuf[2 * block + c], preferred_element_type=jnp.float32
                ).astype(jnp.bfloat16)
            return 0

        lax.fori_loop(0, count, body, 0)

    R = {(k, s): links.ticket() for s in range(2) for k in ("x", "yp", "ym", "h0", "h1", "zyp0", "zyp1", "zym0", "zym1", "zx")}

    def wide(ref):
        return ref[...].astype(jnp.float32)

    def open_sums(s):
        products(s, 6, 1)
        links.start(R["x", s], terms.at[term(1, 2, s)], from_x.at[s], "xh")
        products(s, 5, 1)
        links.start(R["yp", s], terms.at[term(1, 1, s)], from_y.at[s], "yp")
        products(s, 7, 1)
        links.start(R["ym", s], terms.at[term(1, 3, s)], from_y.at[2 + s], "ym")
        products(s, 0, 5)

    def far(s):
        links.arrive(R["x", s], from_x.at[s])
        here = terms.at[term(0, 2, s)]
        here[...] = (wide(here) + wide(from_x.at[s])).astype(jnp.bfloat16)
        for c, to in ((0, "yp"), (1, "ym")):
            links.start(R[f"h{c}", s], here.at[:, cut[c]], halves.at[2 * c + s], to)
        links.start(R["zyp1", s], terms.at[term(0, 1, s), :, cut[1]], last_y.at[s, :, cut[1]], "yp")
        links.start(R["zym0", s], terms.at[term(0, 3, s), :, cut[0]], last_y.at[2 + s, :, cut[0]], "ym")

    def over(s):
        links.arrive(R["yp", s], from_y.at[s])
        links.arrive(R["ym", s], from_y.at[2 + s])
        here = terms.at[term(1, 0, s)]
        here[...] = (wide(here) + wide(from_y.at[s]) + wide(from_y.at[2 + s])).astype(jnp.bfloat16)
        links.start(R["zx", s], here, last_x.at[s], "xh")

    def close(s):
        for c, dy, k, to in ((0, 1, "zyp0", "yp"), (1, 3, "zym1", "ym")):
            links.arrive(R[f"h{c}", s], halves.at[2 * c + s])
            here = terms.at[term(0, dy, s), :, cut[c]]
            here[...] = (wide(here) + wide(halves.at[2 * c + s])).astype(jnp.bfloat16)
            links.start(R[k, s], here, last_y.at[2 * c + s, :, cut[c]], to)

    def result(s):
        links.arrive(R["zx", s], last_x.at[s])
        for c in range(2):
            links.arrive(R[f"zyp{c}", s], last_y.at[s, :, cut[c]])
            links.arrive(R[f"zym{c}", s], last_y.at[2 + s, :, cut[c]])
        total = wide(terms.at[term(0, 0, s)]) + wide(last_x.at[s]) + wide(last_y.at[s]) + wide(last_y.at[2 + s])
        mixed[s] = total.astype(jnp.bfloat16)

    for s in range(2):
        kv[s]["partner"](0)
        kv[s]["forward"]()
        kv[s]["partner"](1)
    o["partner"](0)
    o["partner"](1)
    for s in range(2):
        kv[s]["across"]()
    o["across"]()
    kv[0]["shared"](own_column)
    look(0, True)
    kv[0]["sides"]()
    kv[1]["sides"]()
    kv[0]["last"]()
    kv[1]["last"]()
    kv[0]["shared"](other_column)
    look(0, False)
    o["sides"]()
    o["last"]()
    o["shared"](own_column + other_column)
    open_sums(0)
    kv[1]["shared"](own_column)
    look(1, True)
    far(0)
    over(0)
    kv[1]["shared"](other_column)
    look(1, False)
    open_sums(1)
    close(0)
    far(1)
    over(1)
    result(0)
    close(1)
    result(1)
    links.finish()


def per_device(tokens, norm_gain, span_order, w_query, w_key, value_weight, w_out):
    n_ctx, n_tp = 16, 8
    seqs, rows, depth = tokens.shape
    qw = w_query.shape[1]
    width = qw + w_key.shape[1] + value_weight.shape[1]
    heads = qw // HEAD_DIM
    bf16, f32, i32 = jnp.bfloat16, jnp.float32, jnp.int32
    order = jnp.arange(HEAD_DIM // 2, dtype=f32)
    freqs = jnp.exp(-(2.0 * order / HEAD_DIM) * math.log(theta_base))
    freqs = jnp.concatenate([freqs, freqs])[None]
    anyspace = pl.BlockSpec(memory_space=pl.ANY)
    vmem = pl.BlockSpec(memory_space=pltpu.VMEM)
    return pl.pallas_call(
        mix_kernel,
        out_shape=jax.ShapeDtypeStruct(tokens.shape, bf16),
        in_specs=[anyspace] * 5 + [pl.BlockSpec(memory_space=pltpu.SMEM)] + [vmem] * 2,
        out_specs=vmem,
        scratch_shapes=[
            pltpu.VMEM((seqs, rows, HEAD_DIM), f32),
            pltpu.VMEM((seqs, rows, HEAD_DIM), f32),
            pltpu.VMEM((seqs, rows, 128), i32),
            pltpu.VMEM((2 * seqs, 1, 8 * rows), i32),
            pltpu.VMEM((n_tp * seqs, rows, depth), bf16),
            pltpu.VMEM((n_ctx, w_query.shape[0], width), bf16),
            pltpu.VMEM((seqs * rows, width), f32),
            pltpu.VMEM((n_tp, seqs, 8, rows), f32),
            pltpu.VMEM((seqs * rows, 128), f32),
            pltpu.VMEM((n_ctx, *w_out.shape), bf16),
            pltpu.VMEM((seqs * n_ctx, 2 * rows, HEAD_DIM), bf16),
            pltpu.VMEM((seqs * heads, rows, HEAD_DIM), bf16),
            pltpu.VMEM((heads, rows, 128), f32),
            pltpu.VMEM((heads, rows, 2 * HEAD_DIM), f32),
            pltpu.VMEM((seqs, rows, qw), bf16),
            pltpu.VMEM((n_tp * seqs, rows, depth), bf16),
            pltpu.VMEM((seqs, rows, depth), bf16),
            pltpu.VMEM((2 * seqs, rows, depth), bf16),
            pltpu.VMEM((2 * seqs, rows, depth // 2), bf16),
            pltpu.VMEM((2 * seqs, rows, depth), bf16),
            pltpu.VMEM((seqs, rows, depth), bf16),
            pltpu.SemaphoreType.DMA((144,)),
            pltpu.SemaphoreType.DMA((144,)),
            pltpu.SemaphoreType.DMA((5,)),
        ],
        compiler_params=pltpu.CompilerParams(
            collective_id=0, has_side_effects=True, vmem_limit_bytes=63 * 2**20
        ),
    )(tokens, w_query, w_key, value_weight, w_out, span_order, norm_gain.reshape(n_tp, 1, depth), freqs)


def solution(mesh):
    placed = (
        P(None, "ctx", "tp"),
        P(),
        P(),
        P("ctx", "tp"),
        P("ctx", "tp"),
        P("ctx", "tp"),
        P("tp", "ctx"),
    )
    return jax.shard_map(
        per_device, mesh=mesh, in_specs=placed, out_specs=P(None, "ctx", "tp"), check_vma=False
    )
```
